128 devices in a mesh: rows: 16 (over z, x_lo, core), aux: 8 (over x_hi, y).
Axes of the slice: x: 4 (x_hi: 2, x_lo: 2; x = x_hi * 2 + x_lo), y: 4, z: 4, core: 2. Of those that a mesh axis runs over, the one named last changes fastest.
Arguments:
- pair_coeffs: float32 [36000, 16384], P('aux', 'rows'), may hold values from -0.046875 to 0.046875
- pair_gaps: float32 [16384], P('rows'), may hold values from 0.2 to 20
- trial_vectors: float32 [36000, 128], P('aux'), may hold values from -0.03125 to 0.03125
Outputs:
- vectors_out: float32 [36000, 128], P('aux')
- rayleigh: float32 [128, 128], replicated
The draws below stay inside these ranges and needn't reach their ends.
All inputs are finite; a program needn't handle non-finite values.
Results may differ from the reference program's by a relative error of at most 0.00011.
Values sent between devices are 32-bit elements; how exact they have to be, the bound alone decides.
No kernel may reach another device: no remote copies, remote signals or barrier semaphores. Data moves between devices by JAX's collectives and lax.ppermute only.
A program may use at most 128 MiB of HBM per device.

```python
import math
import jax
import jax.numpy as jnp
from jax import lax

NAUX = 36000
K = 128
ITERS = 2
PAIRS = 16384


def shard_levels(stream_key, shape, pieces, low, top_value):
    def one(position, shards_of):
        steps = jax.random.uniform(jax.random.fold_in(jax.random.fold_in(stream_key, 6), position), (shards_of,), jnp.float32, low / len(pieces), top_value / len(pieces))
        return jnp.repeat(jnp.exp(steps), shape[position] // shards_of).reshape((-1,) + (1,) * (len(shape) - position - 1))

    factor_of = one(*pieces[0])
    for cut in pieces[1:]:
        factor_of = factor_of * one(*cut)
    return factor_of


def normal_values(own_key, dims, deviation, bound, pieces=(), kind=jnp.bfloat16):
    drawn = deviation * jax.random.normal(own_key, dims, jnp.float32)
    if pieces:
        drawn = drawn * shard_levels(own_key, dims, pieces, -0.22, 0.18)
    return jnp.clip(drawn, -bound, bound).astype(kind)


def setup_inputs(seed: int = 0) -> dict:
    arg_keys = jax.random.split(jax.random.key(seed), 4)
    return {
        "pair_coeffs": normal_values(arg_keys[0], (NAUX, PAIRS), PAIRS ** -0.5, 0.046875, ((0, 8), (1, 16)), jnp.float32),
        "pair_gaps": jnp.clip(jnp.exp(math.log(20.0) - 4.6051702 * jax.random.uniform(arg_keys[1], (PAIRS,), jnp.float32) ** shard_levels(arg_keys[1], (PAIRS,), ((0, 16),), -0.2, 0.2)), 0.2, 20.0),
        "trial_vectors": normal_values(arg_keys[2], (NAUX, K), NAUX ** -0.5, 0.03125, ((0, 8),), jnp.float32),
    }


def project(pair_coeffs, vectors):
    return lax.dot_general(pair_coeffs.astype(jnp.float32), vectors.astype(jnp.float32), (((0,), (0,)), ((), ())), precision=lax.Precision.HIGHEST, preferred_element_type=jnp.float32)

def reference(pair_coeffs, pair_gaps, trial_vectors):
    highest = lax.Precision.HIGHEST
    weights = 4.0 * pair_gaps / (pair_gaps * pair_gaps + 1.0)
    vectors = trial_vectors
    for step in range(ITERS):
        projected = project(pair_coeffs, vectors)
        scaled = weights[:, None] * projected
        applied = jnp.dot(pair_coeffs.astype(jnp.float32), scaled.astype(jnp.float32), precision=highest, preferred_element_type=jnp.float32)
        correlation = jnp.dot(applied.T.astype(jnp.float32), applied.astype(jnp.float32), precision=highest, preferred_element_type=jnp.float32)
        factor = jnp.linalg.cholesky(correlation)
        vectors = jax.scipy.linalg.solve_triangular(factor, applied.T, lower=True).T
    final_proj = project(pair_coeffs, vectors)
    rayleigh = jnp.dot(final_proj.T.astype(jnp.float32), (weights[:, None] * final_proj).astype(jnp.float32), precision=highest, preferred_element_type=jnp.float32)
    return (vectors, rayleigh)
```

```python
import jax
import jax.numpy as jnp
from jax import lax
from jax.experimental import pallas as pl
from jax.experimental.pallas import tpu as pltpu
from jax.sharding import Mesh, PartitionSpec as P


F32 = jnp.float32
BF16 = jnp.bfloat16
HIGHEST = lax.Precision.HIGHEST

NAUX_L = 4500
PAIRS_L = 1024
K = 128
CHUNK = 768
PIECE = 96
CHUNKS = 6
ROWS = CHUNK * CHUNKS
TAIL = NAUX_L - CHUNK * (CHUNKS - 1)
CHUNK_J = PAIRS_L // 8

ROW_ORDERS = ((0, 1, 2), (1, 2, 0), (2, 0, 1))


def row_rel(q, p):
    return sum(((p >> (2 - t)) & 1) << ROW_ORDERS[q][t] for t in range(3))


AUX_SEND = ((4, 5, 6, 7), (2, 3, 6, 7))
AUX_KEEP = ((0, 1, 2, 3), (0, 1, 4, 5))


def split(x):
    hi = x.astype(BF16)
    return hi, (x - hi.astype(F32)).astype(BF16)


def dot(a, b, ca, cb, precision=None):
    return lax.dot_general(
        a, b, (((ca,), (cb,)), ((), ())), precision=precision, preferred_element_type=F32
    )


def kernel_call(body, outs, smem, hbm, vmem, scratch=(), limit=30 << 20, name=None):
    spec = pl.BlockSpec(memory_space=pltpu.VMEM)
    return pl.pallas_call(
        body,
        out_shape=[pltpu.VMEM(s, d) for s, d in outs],
        in_specs=[pl.BlockSpec(memory_space=pltpu.SMEM)] * len(smem)
        + [pl.BlockSpec(memory_space=pl.ANY)] * len(hbm)
        + [spec] * len(vmem),
        out_specs=[spec] * len(outs),
        scratch_shapes=list(scratch),
        compiler_params=pltpu.CompilerParams(vmem_limit_bytes=limit),
        name=name,
    )(*smem, *hbm, *[pltpu.with_memory_space_constraint(v, pltpu.VMEM) for v in vmem])


def transposed_halves(v, vt_ref):
    hi, lo = split(v.T)
    vt_ref[0:K, :] = hi
    vt_ref[K : 2 * K, :] = lo


def project_chunk(vt_ref, bhi_ref, blo_ref, acc_ref, row0, first):
    vt = vt_ref[...]
    for n in range(4):
        part = dot(vt, bhi_ref[n, pl.ds(row0, CHUNK), :], 1, 0) + dot(
            vt, blo_ref[n, pl.ds(row0, CHUNK), :], 1, 0
        )
        part = part[0:K, :] + part[K : 2 * K, :]

        @pl.when(first)
        def _():
            acc_ref[2 * n] = part[:, 0:128]
            acc_ref[2 * n + 1] = part[:, 128:256]

        @pl.when(jnp.logical_not(first))
        def _():
            acc_ref[2 * n] += part[:, 0:128]
            acc_ref[2 * n + 1] += part[:, 128:256]


def put_projection(meta, acc_ref, gram, sends, keeps):
    me = meta[4]
    for q in range(2):
        lo = 64 * q
        for slot, pos in enumerate(AUX_SEND[q]):
            sends[q][slot] = acc_ref[pos ^ me, lo : lo + 64, :]
        for slot, pos in enumerate(AUX_KEEP[q]):
            keeps[q][slot] = acc_ref[pos ^ me, lo : lo + 64, :]
        if gram is not None:
            sends[q][4] = gram[lo : lo + 64, :]
            keeps[q][4] = gram[lo : lo + 64, :]


def first_projection(meta, coeffs, vectors):
    def body(
        meta, b_hbm, v_hbm, bhi, blo, s0, s1, k0, k1, bbuf, vbuf, btail, vtail, vt, acc, sems
    ):
        def copies(i):
            last = i == CHUNKS - 1
            rows = pl.ds(i * CHUNK, TAIL if last else CHUNK)
            return (
                pltpu.make_async_copy(b_hbm.at[rows], btail if last else bbuf.at[i], sems.at[0, i]),
                pltpu.make_async_copy(v_hbm.at[rows], vtail if last else vbuf.at[i], sems.at[1, i]),
            )

        for i in range(CHUNKS):
            for c in copies(i):
                c.start()
        for i in range(CHUNKS):
            for c in copies(i):
                c.wait()
            slot = i
            if i == CHUNKS - 1:
                slot = 0
                bbuf[0, TAIL // 8 * 8 :, :] = jnp.zeros((CHUNK - TAIL // 8 * 8, PAIRS_L), F32)
                vbuf[0, TAIL // 8 * 8 :, :] = jnp.zeros((CHUNK - TAIL // 8 * 8, K), F32)
                bbuf[0, 0:TAIL, :] = btail[...]
                vbuf[0, 0:TAIL, :] = vtail[...]
            transposed_halves(vbuf[slot], vt)
            for n in range(4):
                hi, lo = split(bbuf[slot, :, 256 * n : 256 * n + 256])
                bhi[n, CHUNK * i : CHUNK * (i + 1), :] = hi
                blo[n, CHUNK * i : CHUNK * (i + 1), :] = lo
                part = dot(vt[...], hi, 1, 0) + dot(vt[...], lo, 1, 0)
                part = part[0:K, :] + part[K : 2 * K, :]
                if i == 0:
                    acc[2 * n] = part[:, 0:128]
                    acc[2 * n + 1] = part[:, 128:256]
                else:
                    acc[2 * n] += part[:, 0:128]
                    acc[2 * n + 1] += part[:, 128:256]
        put_projection(meta, acc, None, (s0, s1), (k0, k1))

    piece = ((4, 64, 128), F32)
    halves = ((4, ROWS, 256), BF16)
    return kernel_call(
        body,
        [halves, halves, piece, piece, piece, piece],
        [meta],
        [coeffs, vectors],
        [],
        scratch=[
            pltpu.VMEM((CHUNKS - 1, CHUNK, PAIRS_L), F32),
            pltpu.VMEM((CHUNKS - 1, CHUNK, K), F32),
            pltpu.VMEM((TAIL, PAIRS_L), F32),
            pltpu.VMEM((TAIL, K), F32),
            pltpu.VMEM((2 * K, CHUNK), BF16),
            pltpu.VMEM((8, K, 128), F32),
            pltpu.SemaphoreType.DMA((2, CHUNKS)),
        ],
        limit=40 << 20,
        name="first_projection",
    )


def projection(meta, bhi, blo, mine, theirs, keep_vectors):
    def body(meta, bhi, blo, *rest):
        ins, rest = rest[:18], rest[18:]
        s0, s1, k0, k1 = rest[:4]
        rest = rest[4:]
        if keep_vectors:
            vall, rest = rest[0], rest[1:]
        else:
            vall, rest = rest[-1], rest[:-1]
        vt, acc, gacc = rest
        me = meta[0] + 2 * meta[1] + 4 * meta[2]
        for cr in range(2):
            core = cr ^ meta[3]
            for q in range(3):
                low, mid, high = ins[9 * cr + 3 * q : 9 * cr + 3 * q + 3]
                for p in range(8):
                    src = low[p] if p < 2 else mid[p - 2] if p < 4 else high[p - 4]
                    vall[24 * core + 8 * q + (row_rel(q, p) ^ me)] = src

        def chunk(i, carry):
            v = vall[pl.ds(8 * i, 8)].reshape(CHUNK, K)
            transposed_halves(v, vt)
            first = i == 0
            project_chunk(vt, bhi, blo, acc, pl.multiple_of(i * CHUNK, CHUNK), first)
            g = dot(vt[...], vt[...], 1, 1)

            @pl.when(first)
            def _():
                gacc[...] = g

            @pl.when(jnp.logical_not(first))
            def _():
                gacc[...] += g

            return carry

        lax.fori_loop(0, CHUNKS, chunk, 0)
        g = gacc[...]
        gram = (g[0:K, 0:K] + g[K : 2 * K, K : 2 * K]) + (g[0:K, K : 2 * K] + g[K : 2 * K, 0:K])
        put_projection(meta, acc, gram, (s0, s1), (k0, k1))

    piece = ((5, 64, 128), F32)
    vectors = (8 * CHUNKS, PIECE, K)
    outs = [piece] * 4 + ([(vectors, F32)] if keep_vectors else [])
    scratch = [
        pltpu.VMEM((2 * K, CHUNK), BF16),
        pltpu.VMEM((8, K, 128), F32),
        pltpu.VMEM((2 * K, 2 * K), F32),
    ] + ([] if keep_vectors else [pltpu.VMEM(vectors, F32)])
    return kernel_call(
        body, outs, [meta], [], [bhi, blo, *mine, *theirs], scratch=scratch, name="projection"
    )


def apply_half(meta, bhi, blo, other, scaled_in, make_scaled):
    def body(meta, bhi, blo, *rest):
        if make_scaled:
            u, rx, a0, a1, b0, b1, out, st, part = rest
            me = meta[4]

            def put(pos, row0, value):
                hi, lo = split(value)
                rows = value.shape[0]
                st[pos ^ me, row0 : row0 + rows, :] = hi
                st[pos ^ me, K + row0 : K + row0 + rows, :] = lo

            put(0, 0, u[...])
            put(1, 0, rx[...])
            for t in range(2):
                put(2 + t, 0, a0[t])
                put(4 + t, 64, a1[t])
            for t in range(4):
                put(AUX_SEND[0][t], 0, b0[t])
                put(AUX_SEND[1][t], 64, b1[t])
        else:
            st, out, part = rest
        me = meta[0] + 2 * meta[1] + 4 * meta[2]
        half = (1 - meta[3]) if other else meta[3]
        rhs = [jnp.concatenate([st[2 * n], st[2 * n + 1]], axis=1) for n in range(4)]
        for q in range(3):
            row0 = pl.multiple_of(half * 3 * CHUNK + q * CHUNK, CHUNK)
            res = None
            for ref in (bhi, blo):
                for n in range(4):
                    d = dot(ref[n, pl.ds(row0, CHUNK), :], rhs[n], 1, 1)
                    res = d if res is None else res + d
            part[...] = (res[:, 0:K] + res[:, K : 2 * K]).reshape(8, PIECE, K)
            for p in range(8):
                out[8 * q + p] = part[row_rel(q, p) ^ me]

    outs = [((24, PIECE, K), F32)]
    if make_scaled:
        outs.append(((8, 2 * K, 128), BF16))
    return kernel_call(
        body,
        outs,
        [meta],
        [],
        [bhi, blo, *scaled_in],
        scratch=[pltpu.VMEM((8, PIECE, K), F32)],
        name="apply_other" if other else "apply_own",
    )


def add_cores(keep, got):
    def body(keep, got, *outs):
        for q in range(3):
            outs[q][...] = keep[8 * q + 4 : 8 * q + 8] + got[8 * q + 4 : 8 * q + 8]
            outs[3 + q][...] = keep[8 * q : 8 * q + 4] + got[8 * q : 8 * q + 4]

    return kernel_call(body, [((4, PIECE, K), F32)] * 6, [], [], [keep, got], name="add_cores")


def sum_pieces(parts, inverse):
    def body(*refs):
        outs = refs[-3:]
        for q in range(3):
            k, r1, r2, r3 = refs[4 * q : 4 * q + 4]
            s = (k[0] + r1[0]) + (r2[0] + r3[0])
            if inverse is not None:
                s = dot(s, refs[12][...], 1, 1, HIGHEST)
            outs[q][0] = s

    extra = [] if inverse is None else [inverse]
    return kernel_call(body, [((1, PIECE, K), F32)] * 3, [], [], [*parts, *extra], name="sum_pieces")


def inverse_factor(gram):
    def body(g_ref, out_ref, gs, ws):
        lane = lax.broadcasted_iota(jnp.int32, (K, K), 1)
        sub = lax.broadcasted_iota(jnp.int32, (K, K), 0)
        gs[...] = g_ref[...]
        ws[...] = jnp.where(lane == sub, 1.0, 0.0).astype(F32)

        def step(k, carry):
            g, w = gs[...], ws[...]
            row = gs[pl.ds(k, 1), :]
            wrow = ws[pl.ds(k, 1), :]
            col = jnp.sum(jnp.where(lane == k, g, 0.0), axis=1, keepdims=True)
            pivot = jnp.sum(jnp.where(lane[0:1] == k, row, 0.0), axis=1, keepdims=True)
            f = jnp.where(sub[:, 0:1] > k, col / pivot, 0.0)
            gs[...] = g - f * row
            ws[...] = w - f * wrow
            return carry

        lax.fori_loop(0, K, step, 0)
        d = jnp.sum(jnp.where(lane == sub, gs[...], 0.0), axis=1, keepdims=True)
        out_ref[...] = ws[...] / jnp.sqrt(d)

    return kernel_call(
        body,
        [((K, K), F32)],
        [],
        [],
        [gram],
        scratch=[pltpu.VMEM((K, K), F32), pltpu.VMEM((K, K), F32)],
        name="inverse_factor",
    )[0]


def finish_vectors(vall, inverse):
    def body(v, inv, out, buf, tail, sem):
        ihi, ilo = split(inv[...])
        rhs = jnp.concatenate([ihi, ilo], axis=0)

        def copy(i):
            last = i == CHUNKS - 1
            rows = pl.ds(i * CHUNK, TAIL if last else CHUNK)
            return pltpu.make_async_copy(tail if last else buf.at[i], out.at[rows], sem.at[i])

        for i in range(CHUNKS):
            vhi, vlo = split(v[8 * i : 8 * i + 8].reshape(CHUNK, K))
            r = dot(vhi, rhs, 1, 1) + dot(vlo, rhs, 1, 1)
            r = r[:, 0:K] + r[:, K : 2 * K]
            if i == CHUNKS - 1:
                tail[...] = r[0:TAIL]
            else:
                buf[i] = r
            copy(i).start()
        for i in range(CHUNKS):
            copy(i).wait()

    spec = pl.BlockSpec(memory_space=pltpu.VMEM)
    return pl.pallas_call(
        body,
        out_shape=jax.ShapeDtypeStruct((NAUX_L, K), F32),
        in_specs=[spec, spec],
        out_specs=pl.BlockSpec(memory_space=pl.ANY),
        scratch_shapes=[
            pltpu.VMEM((CHUNKS - 1, CHUNK, K), F32),
            pltpu.VMEM((TAIL, K), F32),
            pltpu.SemaphoreType.DMA((CHUNKS,)),
        ],
        compiler_params=pltpu.CompilerParams(vmem_limit_bytes=30 << 20),
        name="finish_vectors",
    )(
        pltpu.with_memory_space_constraint(vall, pltpu.VMEM),
        pltpu.with_memory_space_constraint(inverse, pltpu.VMEM),
    )


def exchange(value, axis, mask):
    n = lax.axis_size(axis)
    return lax.ppermute(value, axis, [(i, i ^ mask) for i in range(n)])


ROW_DIMS = (("z", 1), ("z", 3), ("xl", 1))


def over_rows(own, got):
    parts = add_cores(own, got)
    sends, keeps = parts[:3], parts[3:]
    dims = [[ROW_DIMS[ROW_ORDERS[q][t]] for t in range(3)] for q in range(3)]
    r1 = [exchange(sends[q], *dims[q][0]) for q in range(3)]
    r2 = [exchange(keeps[q][2:4] + r1[q][2:4], *dims[q][1]) for q in range(3)]
    r3 = [exchange(keeps[q][1:2] + r1[q][1:2] + r2[q][1:2], *dims[q][2]) for q in range(3)]
    out = []
    for q in range(3):
        out += [keeps[q], r1[q], r2[q], r3[q]]
    return out


def gather_rows(pieces):
    dims = [[ROW_DIMS[ROW_ORDERS[q][t]] for t in range(3)] for q in range(3)]
    t3 = [exchange(pieces[q], *dims[q][2]) for q in range(3)]
    low = [jnp.concatenate([pieces[q], t3[q]], axis=0) for q in range(3)]
    mid = [exchange(low[q], *dims[q][1]) for q in range(3)]
    four = [jnp.concatenate([low[q], mid[q]], axis=0) for q in range(3)]
    high = [exchange(four[q], *dims[q][0]) for q in range(3)]
    mine, theirs = [], []
    for q in range(3):
        mine += [low[q], mid[q], high[q]]
    theirs = [exchange(b, "c", 1) for b in mine]
    return mine, theirs


def reduce_aux(sends, keeps):
    s0, s1 = sends
    k0, k1 = keeps
    has_gram = s0.shape[0] == 5
    r0 = exchange(s0, "y", 1)
    r1 = exchange(s1, "y", 3)
    t0 = exchange(k0[2:] + r0[2:], "y", 3)
    t1 = exchange(k1[2:] + r1[2:], "y", 1)

    def gram_of(k, r, t):
        return k[4] + r[4] + t[2]

    nxt = [k0[1] + r0[1] + t0[1], k1[1] + r1[1] + t1[1]]
    if has_gram:
        g0, g1 = gram_of(k0, r0, t0), gram_of(k1, r1, t1)
        nxt += [g0, g1]
    x = exchange(jnp.concatenate(nxt, axis=0), "xh", 1)
    own = jnp.concatenate([k0[0] + r0[0] + t0[0], k1[0] + r1[0] + t1[0]], axis=0) + x[0:K]
    gram = jnp.concatenate([g0, g1], axis=0) + x[K:] if has_gram else None
    return own, gram


def gather_aux(u):
    rx = exchange(u, "xh", 1)
    both = jnp.stack([u, rx], axis=0)
    a0 = exchange(both[:, 0:64], "y", 3)
    a1 = exchange(both[:, 64:], "y", 1)
    b0 = exchange(jnp.concatenate([both[:, 0:64], a0], axis=0), "y", 1)
    b1 = exchange(jnp.concatenate([both[:, 64:], a1], axis=0), "y", 3)
    return u, rx, a0, a1, b0, b1


def sum_all(value):
    value = value + exchange(value, "c", 1)
    for axis in ("z", "y"):
        a = exchange(value, axis, 1)
        value = value + a
        value = value + exchange(value, axis, 3)
    value = value + exchange(value, "xl", 1)
    return value + exchange(value, "xh", 1)


def shards(pair_coeffs, pair_gaps, trial_vectors):
    z, xl, core = lax.axis_index("z"), lax.axis_index("xl"), lax.axis_index("c")
    xh, y = lax.axis_index("xh"), lax.axis_index("y")

    def bits(i):
        b = (i >> 1) & 1
        return (i & 1) ^ b, b

    z1, z3 = bits(z)
    y1, y3 = bits(y)
    aux = 4 * y1 + 2 * y3 + xh
    meta = jnp.stack([z1, z3, xl, core, aux]).astype(jnp.int32)
    gaps = lax.dynamic_slice_in_dim(pair_gaps, aux * CHUNK_J, CHUNK_J)
    weights = (4.0 * gaps / (gaps * gaps + 1.0))[None, :]

    bhi, blo, s0, s1, k0, k1 = first_projection(meta, pair_coeffs, trial_vectors)
    inverse = None
    for step in range(2):
        own, gram = reduce_aux((s0, s1), (k0, k1))
        if gram is not None:
            inverse = inverse_factor(gram)
        scaled = gather_aux(own * weights)
        send, st = apply_half(meta, bhi, blo, True, scaled, True)
        got = exchange(send, "c", 1)
        (keep,) = apply_half(meta, bhi, blo, False, [st], False)
        parts = over_rows(keep, got)
        pieces = sum_pieces(parts, inverse)
        mine, theirs = gather_rows(pieces)
        s0, s1, k0, k1, *vall = projection(meta, bhi, blo, mine, theirs, step == 1)
    own, gram = reduce_aux((s0, s1), (k0, k1))
    inverse = inverse_factor(gram)
    local = dot(own * weights, own, 1, 1, HIGHEST)
    total = sum_all(local)
    rayleigh = dot(dot(inverse, total, 1, 0, HIGHEST), inverse, 1, 1, HIGHEST)
    vectors_out = finish_vectors(vall[0], inverse)
    return vectors_out, rayleigh


def solution(mesh):
    cube = Mesh(mesh.devices.reshape(4, 2, 2, 2, 4), ("z", "xl", "c", "xh", "y"))
    rows, aux = ("z", "xl", "c"), ("xh", "y")
    return jax.shard_map(
        shards,
        mesh=cube,
        in_specs=(P(aux, rows), P(rows), P(aux, None)),
        out_specs=(P(aux, None), P()),
        check_vma=False,
    )
```

```python
import jax
import jax.numpy as jnp
from jax import lax
from jax.experimental import pallas as pl
from jax.experimental.pallas import tpu as pltpu
from jax.sharding import Mesh, PartitionSpec as P


F32 = jnp.float32
BF16 = jnp.bfloat16
HIGHEST = lax.Precision.HIGHEST

NAUX_L = 4500
PAIRS_L = 1024
K = 128
CHUNK = 768
CHUNKS = 6
ROWS = CHUNK * CHUNKS
HALF = ROWS // 2
TAIL = NAUX_L - CHUNK * (CHUNKS - 1)
CHIPS = 8
PIECE = HALF // CHIPS
PAIRS_J = PAIRS_L // CHIPS
GRAM_J = K // CHIPS


def split(x):
    hi = x.astype(BF16)
    return hi, (x - hi.astype(F32)).astype(BF16)


def dot(a, b, ca, cb, precision=None):
    return lax.dot_general(
        a, b, (((ca,), (cb,)), ((), ())), precision=precision, preferred_element_type=F32
    )


VMEM_SPEC = pl.BlockSpec(memory_space=pltpu.VMEM)


def kernel_call(body, outs, smem, hbm, vmem, scratch=(), limit=12 << 20, name=None):
    return pl.pallas_call(
        body,
        out_shape=[pltpu.VMEM(s, d) for s, d in outs],
        in_specs=[pl.BlockSpec(memory_space=pltpu.SMEM)] * len(smem)
        + [pl.BlockSpec(memory_space=pl.ANY)] * len(hbm)
        + [VMEM_SPEC] * len(vmem),
        out_specs=[VMEM_SPEC] * len(outs),
        scratch_shapes=list(scratch),
        compiler_params=pltpu.CompilerParams(vmem_limit_bytes=limit),
        name=name,
    )(*smem, *hbm, *[pltpu.with_memory_space_constraint(v, pltpu.VMEM) for v in vmem])


def transposed_halves(v):
    hi, lo = split(v.T)
    return jnp.concatenate([hi, lo], axis=0)


def fold(x):
    return x[0:K, :] + x[K : 2 * K, :]


def first_projection(coeffs, vectors):
    def body(b_hbm, v_hbm, bhi, blo, out, bbuf, vbuf, btail, vtail, sems):
        def copies(i):
            last = i == CHUNKS - 1
            rows = pl.ds(i * CHUNK, TAIL if last else CHUNK)
            return (
                pltpu.make_async_copy(b_hbm.at[rows], btail if last else bbuf.at[i], sems.at[0, i]),
                pltpu.make_async_copy(v_hbm.at[rows], vtail if last else vbuf.at[i], sems.at[1, i]),
            )

        for i in range(CHUNKS):
            for c in copies(i):
                c.start()
        for i in range(CHUNKS):
            for c in copies(i):
                c.wait()
            slot = i
            if i == CHUNKS - 1:
                slot = 0
                bbuf[0, TAIL // 8 * 8 :, :] = jnp.zeros((CHUNK - TAIL // 8 * 8, PAIRS_L), F32)
                vbuf[0, TAIL // 8 * 8 :, :] = jnp.zeros((CHUNK - TAIL // 8 * 8, K), F32)
                bbuf[0, 0:TAIL, :] = btail[...]
                vbuf[0, 0:TAIL, :] = vtail[...]
            vt = transposed_halves(vbuf[slot])
            for n in range(4):
                hi, lo = split(bbuf[slot, :, 256 * n : 256 * n + 256])
                bhi[n, CHUNK * i : CHUNK * (i + 1), :] = hi
                blo[n, CHUNK * i : CHUNK * (i + 1), :] = lo
                part = fold(dot(vt, hi, 1, 0) + dot(vt, lo, 1, 0))
                for t in range(2):
                    value = part[:, 128 * t : 128 * t + 128]
                    out[2 * n + t] = value if i == 0 else out[2 * n + t] + value

    halves = ((4, ROWS, 256), BF16)
    return kernel_call(
        body,
        [halves, halves, ((CHIPS, K, PAIRS_J), F32)],
        [],
        [coeffs, vectors],
        [],
        scratch=[
            pltpu.VMEM((CHUNKS - 1, CHUNK, PAIRS_L), F32),
            pltpu.VMEM((CHUNKS - 1, CHUNK, K), F32),
            pltpu.VMEM((TAIL, PAIRS_L), F32),
            pltpu.VMEM((TAIL, K), F32),
            pltpu.SemaphoreType.DMA((2, CHUNKS)),
        ],
        limit=26 << 20,
        name="first_projection",
    )


def project_half(meta, bhi, blo, v, so_far, gram_rows=GRAM_J):
    def body(meta, bhi, blo, v, *rest):
        if so_far is None:
            acc, gacc = rest
            half = meta[0]
        else:
            acc0, gacc0, out, acc, gacc = rest
            half = 1 - meta[0]
        for i in range(3):
            row0 = pl.multiple_of(half * HALF + i * CHUNK, CHUNK)
            vt = transposed_halves(v[CHUNK * i : CHUNK * (i + 1), :])
            for n in range(4):
                part = fold(
                    dot(vt, bhi[n, pl.ds(row0, CHUNK), :], 1, 0)
                    + dot(vt, blo[n, pl.ds(row0, CHUNK), :], 1, 0)
                )
                for t in range(2):
                    value = part[:, 128 * t : 128 * t + 128]
                    j = 2 * n + t
                    if i > 0:
                        value = acc[j] + value
                    if so_far is not None and i == 2:
                        out[j, 0:K, :] = acc0[j] + value
                    else:
                        acc[j] = value
            g = dot(vt, vt, 1, 1)
            gacc[...] = g if i == 0 else gacc[...] + g
        if so_far is not None:
            g = gacc[...] + gacc0[...]
            gram = (g[0:K, 0:K] + g[K:, K:]) + (g[0:K, K:] + g[K:, 0:K])
            for j in range(CHIPS):
                first = GRAM_J * j if gram_rows < K else 0
                out[j, K:, :] = gram[first : first + gram_rows, :]

    acc = ((CHIPS, K, PAIRS_J), F32)
    gacc = ((2 * K, 2 * K), F32)
    if so_far is None:
        return kernel_call(body, [acc, gacc], [meta], [], [bhi, blo, v], name="project_own")
    return kernel_call(
        body,
        [((CHIPS, K + gram_rows, PAIRS_J), F32)],
        [meta],
        [],
        [bhi, blo, v, *so_far],
        scratch=[pltpu.VMEM(*acc), pltpu.VMEM(*gacc)],
        name="project_other",
    )


def sum_aux(parts, weights, copies):
    rows = parts.shape[1]

    def body(p, w, *outs):
        s = ((p[0] + p[1]) + (p[2] + p[3])) + ((p[4] + p[5]) + (p[6] + p[7]))
        piece = s[0:K] * w[...]
        if copies:
            for j in range(CHIPS):
                outs[0][j, 0:K, :] = piece
                if rows > K:
                    outs[0][j, K:, :] = s[K:]
        else:
            outs[0][...] = dot(piece, s[0:K], 1, 1, HIGHEST)
            outs[1][...] = s[K:]

    if copies:
        outs = [((CHIPS, rows, PAIRS_J), F32)]
    else:
        outs = [((K, K), F32), ((K, K), F32)]
    return kernel_call(body, outs, [], [], [parts, weights], name="sum_aux")


def apply_half(meta, bhi, blo, other, scaled):
    def body(meta, bhi, blo, s, *rest):
        out = rest[0]
        if other:
            st = rest[1]
            for j in range(CHIPS):
                hi, lo = split(s[j, 0:K, :])
                lanes = slice(128 * (j % 2), 128 * (j % 2) + 128)
                st[j // 2, 0:K, lanes] = hi
                st[j // 2, K : 2 * K, lanes] = lo
        else:
            st = s
        half = (1 - meta[0]) if other else meta[0]
        for i in range(3):
            row0 = pl.multiple_of(half * HALF + i * CHUNK, CHUNK)
            res = None
            for ref in (bhi, blo):
                for n in range(4):
                    d = dot(ref[n, pl.ds(row0, CHUNK), :], st[n], 1, 1)
                    res = d if res is None else res + d
            out[CHUNK * i : CHUNK * (i + 1), :] = res[:, 0:K] + res[:, K : 2 * K]

    outs = [((HALF, K), F32)]
    if other:
        outs.append(((4, 2 * K, 256), BF16))
    return kernel_call(
        body, outs, [meta], [], [bhi, blo, scaled], name="apply_other" if other else "apply_own"
    )


def add_cores(perm, keep, got):
    def body(perm, keep, got, send, kept):
        for p in range(4):
            send[p] = keep[perm[4 + p]] + got[perm[4 + p]]
            kept[p] = keep[perm[p]] + got[perm[p]]

    half = ((4, PIECE, K), F32)
    return kernel_call(body, [half, half], [perm], [], [keep, got], name="add_cores")


def add_slots(first, count, *parts):
    def body(*refs):
        total = refs[0][first : first + count]
        for r in refs[1:-1]:
            total = total + r[first : first + count]
        refs[-1][...] = total

    return kernel_call(body, [((count, PIECE, K), F32)], [], [], list(parts), name="add_slots")[0]


def sum_rows(kept, r1, r2, r3, inverse):
    def body(kept, r1, r2, r3, *refs):
        out = refs[-1]
        s = (kept[0] + r1[0]) + (r2[0] + r3[0])
        if inverse is not None:
            s = dot(s, refs[0][...], 1, 1, HIGHEST)
        for j in range(CHIPS):
            out[j] = s

    extra = [] if inverse is None else [inverse]
    return kernel_call(
        body, [((CHIPS, PIECE, K), F32)], [], [], [kept, r1, r2, r3, *extra], name="sum_rows"
    )[0]


def eliminate(state, begin, end):
    start, stop = begin == 0, end == K

    def body(*refs):
        lane = lax.broadcasted_iota(jnp.int32, (K, K), 1)
        sub = lax.broadcasted_iota(jnp.int32, (K, K), 0)
        if start:
            g_ref, (gs, ws) = refs[0], refs[-2:]
            if len(g_ref.shape) == 2:
                gs[...] = g_ref[...]
            else:
                row0 = g_ref.shape[1] - GRAM_J
                for j in range(CHIPS):
                    gs[GRAM_J * j : GRAM_J * (j + 1), :] = g_ref[j, row0:, :]
            ws[...] = jnp.where(lane == sub, 1.0, 0.0).astype(F32)
        else:
            g_ref, w_ref, (gs, ws) = refs[0], refs[1], refs[-2:]
            gs[...] = g_ref[...]
            ws[...] = w_ref[...]

        def step(h, carry):
            k = 2 * h
            g, w = gs[...], ws[...]
            r0, r1 = gs[pl.ds(k, 1), :], gs[pl.ds(k + 1, 1), :]
            w0, w1 = ws[pl.ds(k, 1), :], ws[pl.ds(k + 1, 1), :]

            def pick(x, at):
                return jnp.sum(jnp.where(lane[0 : x.shape[0]] == at, x, 0.0), axis=1, keepdims=True)

            c0, c1 = pick(g, k), pick(g, k + 1)
            a, b, d = pick(r0, k), pick(r0, k + 1), pick(r1, k + 1)
            ia = 1.0 / a
            m = b * ia
            ip = 1.0 / (d - b * m)
            r1 = r1 - m * r0
            w1 = w1 - m * w0
            f0 = jnp.where(sub[:, 0:1] > k, c0 * ia, 0.0)
            f1 = jnp.where(sub[:, 0:1] > k + 1, (c1 - f0 * b) * ip, 0.0)
            gs[...] = (g - f0 * r0) - f1 * r1
            ws[...] = (w - f0 * w0) - f1 * w1
            return carry

        lax.fori_loop(begin // 2, end // 2, step, 0)
        if stop:
            d = jnp.sum(jnp.where(lane == sub, gs[...], 0.0), axis=1, keepdims=True)
            refs[-3][...] = ws[...] / jnp.sqrt(d)

    square = ((K, K), F32)
    if stop:
        outs, scratch = [square], [pltpu.VMEM(*square), pltpu.VMEM(*square)]
    else:
        outs, scratch = [square, square], []
    return kernel_call(body, outs, [], [], list(state), scratch=scratch, name="eliminate")


def in_between(value, state, cuts):
    state = eliminate(state, cuts[0], cuts[1])
    value, *state = lax.optimization_barrier((value, *state))
    return value, state


def finish_vectors(meta, mine, theirs, inverse):
    def body(meta, mine, theirs, inv, out, both, buf, tail, sem):
        both[meta[0]] = mine[...]
        both[1 - meta[0]] = theirs[...]
        ihi, ilo = split(inv[...])
        rhs = jnp.concatenate([ihi, ilo], axis=0)

        def copy(i):
            last = i == CHUNKS - 1
            rows = pl.ds(i * CHUNK, TAIL if last else CHUNK)
            return pltpu.make_async_copy(tail if last else buf.at[i], out.at[rows], sem.at[i])

        for i in range(CHUNKS):
            start = CHUNK * (i % 3)
            vhi, vlo = split(both[i // 3, start : start + CHUNK, :])
            r = dot(vhi, rhs, 1, 1) + dot(vlo, rhs, 1, 1)
            r = r[:, 0:K] + r[:, K : 2 * K]
            if i == CHUNKS - 1:
                tail[...] = r[0:TAIL]
            else:
                buf[i] = r
            copy(i).start()
        for i in range(CHUNKS):
            copy(i).wait()

    return pl.pallas_call(
        body,
        out_shape=jax.ShapeDtypeStruct((NAUX_L, K), F32),
        in_specs=[pl.BlockSpec(memory_space=pltpu.SMEM)] + [VMEM_SPEC] * 3,
        out_specs=pl.BlockSpec(memory_space=pl.ANY),
        scratch_shapes=[
            pltpu.VMEM((2, HALF, K), F32),
            pltpu.VMEM((CHUNKS - 1, CHUNK, K), F32),
            pltpu.VMEM((TAIL, K), F32),
            pltpu.SemaphoreType.DMA((CHUNKS,)),
        ],
        compiler_params=pltpu.CompilerParams(vmem_limit_bytes=16 << 20),
        name="finish_vectors",
    )(meta, *[pltpu.with_memory_space_constraint(v, pltpu.VMEM) for v in (mine, theirs, inverse)])


def exchange(value, axis, mask):
    n = lax.axis_size(axis)
    return lax.ppermute(value, axis, [(i, i ^ mask) for i in range(n)])


def to_each(value, axes):
    return lax.all_to_all(value, axes, split_axis=0, concat_axis=0, tiled=True)


NEAR = ("z", "xl")
AUX = ("xh", "y")


NEAR_MASK = {("z", 1): 2, ("z", 3): 6, ("xl", 1): 1}
CROSS = ((("z", 1), ("z", 3), ("xl", 1)), (("xl", 1), ("z", 1), ("z", 3)))


def cross(value, step):
    nz, nx = lax.axis_size("z"), lax.axis_size("xl")
    pairs = []
    for z in range(nz):
        for x in range(nx):
            for c in range(2):
                axis, mask = CROSS[c][step]
                to = (z ^ mask, x) if axis == "z" else (z, x ^ mask)
                pairs.append(((z * nx + x) * 2 + c, (to[0] * nx + to[1]) * 2 + c))
    return lax.ppermute(value, ("z", "xl", "c"), pairs)


def positions():
    tables = []
    for core in range(2):
        row = []
        for p in range(8):
            mask = 0
            for t in range(3):
                if (p >> (2 - t)) & 1:
                    mask ^= NEAR_MASK[CROSS[core][t]]
            row.append(mask)
        tables.append(row)
    near = lax.axis_index(NEAR)
    mine = jnp.where(lax.axis_index("c") == 0, jnp.array(tables[0]), jnp.array(tables[1]))
    return (near ^ mine).astype(jnp.int32)


def shards(pair_coeffs, pair_gaps, trial_vectors):
    meta = lax.axis_index("c").astype(jnp.int32)[None]
    aux = lax.axis_index(AUX)
    gaps = lax.dynamic_slice_in_dim(pair_gaps, aux * PAIRS_J, PAIRS_J)
    weights = (4.0 * gaps / (gaps * gaps + 1.0))[None, :]

    perm = positions()
    weights, meta, perm, trial_vectors = lax.optimization_barrier(
        (weights, meta, perm, trial_vectors)
    )
    bhi, blo, parts = first_projection(pair_coeffs, trial_vectors)
    for step in range(2):
        (copies,) = sum_aux(to_each(parts, AUX), weights, True)
        scaled = to_each(copies, AUX)
        send, st = apply_half(meta, bhi, blo, True, scaled)
        got = exchange(send, "c", 1)
        (keep,) = apply_half(meta, bhi, blo, False, st)
        pieces = (CHIPS, PIECE, K)
        first, kept = add_cores(perm, keep.reshape(pieces), got.reshape(pieces))
        r1 = cross(first, 0)
        inverse = None
        if step == 1:
            r1, state = in_between(r1, [scaled], (0, 80))
        r2 = cross(add_slots(2, 2, kept, r1), 1)
        if step == 1:
            r2, state = in_between(r2, state, (80, 112))
        r3 = cross(add_slots(1, 1, kept, r1, r2), 2)
        if step == 1:
            r3, (inverse,) = in_between(r3, state, (112, 128))
        mine = to_each(sum_rows(kept, r1, r2, r3, inverse), NEAR).reshape(HALF, K)
        theirs = exchange(mine, "c", 1)
        so_far = project_half(meta, bhi, blo, mine, None)
        (parts,) = project_half(meta, bhi, blo, theirs, so_far, K if step == 1 else GRAM_J)
    total, gram = sum_aux(to_each(parts, AUX), weights, False)
    total = total + exchange(total, "c", 1)
    state, cuts = [gram], [0, 32, 64, 96, 128]
    for axis in ("z", "y"):
        for mask in (1, 3):
            got = exchange(total, axis, mask)
            got, state = in_between(got, state, cuts)
            cuts = cuts[1:]
            total = total + got
    (inverse,) = state
    got = exchange(total, "xl", 1)
    vectors_out = finish_vectors(meta, mine, theirs, inverse)
    got, vectors_out = lax.optimization_barrier((got, vectors_out))
    total = total + got
    total = total + exchange(total, "xh", 1)
    rayleigh = dot(dot(inverse, total, 1, 0, HIGHEST), inverse, 1, 1, HIGHEST)
    return vectors_out, rayleigh


def solution(mesh):
    cube = Mesh(mesh.devices.reshape(4, 2, 2, 2, 4), ("z", "xl", "c", "xh", "y"))
    return jax.shard_map(
        shards,
        mesh=cube,
        in_specs=(P(AUX, NEAR + ("c",)), P(NEAR + ("c",)), P(AUX, None)),
        out_specs=(P(AUX, None), P()),
        check_vma=False,
    )
```

```python
import jax
import jax.numpy as jnp
from jax import lax
from jax.experimental import pallas as pl
from jax.experimental.pallas import tpu as pltpu
from jax.sharding import Mesh, PartitionSpec as P


F32 = jnp.float32
BF16 = jnp.bfloat16
HIGHEST = lax.Precision.HIGHEST

NAUX_L = 4500
PAIRS_L = 1024
K = 128
CHUNK = 768
CHUNKS = 6
ROWS = CHUNK * CHUNKS
HALF = ROWS // 2
TAIL = NAUX_L - CHUNK * (CHUNKS - 1)
CHIPS = 8
PIECE = HALF // CHIPS
PAIRS_J = PAIRS_L // CHIPS
GRAM_J = K // CHIPS


def split(x):
    hi = x.astype(BF16)
    return hi, (x - hi.astype(F32)).astype(BF16)


def dot(a, b, ca, cb, precision=None):
    return lax.dot_general(
        a, b, (((ca,), (cb,)), ((), ())), precision=precision, preferred_element_type=F32
    )


VMEM_SPEC = pl.BlockSpec(memory_space=pltpu.VMEM)


def cost(us):
    return pl.CostEstimate(flops=int(us * 1.5e8), bytes_accessed=0, transcendentals=0)


def core_of(dev):
    return (dev[0] >> 3) & 1


def near_of(dev):
    return ((dev[0] >> 4) & 1) * 4 + (dev[0] >> 5)


def aux_of(dev):
    return dev[0] & 7


def kernel_call(body, outs, smem, hbm, vmem, scratch=(), limit=12 << 20, us=0.3):
    return pl.pallas_call(
        body,
        out_shape=[pltpu.VMEM(s, d) for s, d in outs],
        in_specs=[pl.BlockSpec(memory_space=pltpu.SMEM)] * len(smem)
        + [pl.BlockSpec(memory_space=pl.ANY)] * len(hbm)
        + [VMEM_SPEC] * len(vmem),
        out_specs=[VMEM_SPEC] * len(outs),
        scratch_shapes=list(scratch),
        compiler_params=pltpu.CompilerParams(vmem_limit_bytes=limit),
        cost_estimate=cost(us),
    )(*smem, *hbm, *[pltpu.with_memory_space_constraint(v, pltpu.VMEM) for v in vmem])


def transposed_halves(v):
    hi, lo = split(v.T)
    return jnp.concatenate([hi, lo], axis=0)


def fold(x):
    return x[0:K, :] + x[K : 2 * K, :]


def first_projection(coeffs, vectors):
    def body(b_hbm, v_hbm, bhi, blo, out, bbuf, vbuf, btail, vtail, sems):
        def copies(i):
            last = i == CHUNKS - 1
            rows = pl.ds(i * CHUNK, TAIL if last else CHUNK)
            return (
                pltpu.make_async_copy(b_hbm.at[rows], btail if last else bbuf.at[i], sems.at[0, i]),
                pltpu.make_async_copy(v_hbm.at[rows], vtail if last else vbuf.at[i], sems.at[1, i]),
            )

        for i in range(CHUNKS):
            for c in copies(i):
                c.start()
        for i in range(CHUNKS):
            for c in copies(i):
                c.wait()
            slot = i
            if i == CHUNKS - 1:
                slot = 0
                bbuf[0, TAIL // 8 * 8 :, :] = jnp.zeros((CHUNK - TAIL // 8 * 8, PAIRS_L), F32)
                vbuf[0, TAIL // 8 * 8 :, :] = jnp.zeros((CHUNK - TAIL // 8 * 8, K), F32)
                bbuf[0, 0:TAIL, :] = btail[...]
                vbuf[0, 0:TAIL, :] = vtail[...]
            vt = transposed_halves(vbuf[slot])
            for n in range(4):
                hi, lo = split(bbuf[slot, :, 256 * n : 256 * n + 256])
                bhi[n, CHUNK * i : CHUNK * (i + 1), :] = hi
                blo[n, CHUNK * i : CHUNK * (i + 1), :] = lo
                part = fold(dot(vt, hi, 1, 0) + dot(vt, lo, 1, 0))
                for t in range(2):
                    value = part[:, 128 * t : 128 * t + 128]
                    out[2 * n + t] = value if i == 0 else out[2 * n + t] + value

    halves = ((4, ROWS, 256), BF16)
    coeffs = pltpu.with_memory_space_constraint(coeffs, pltpu.HBM)
    vectors = pltpu.with_memory_space_constraint(vectors, pltpu.HBM)
    return kernel_call(
        body,
        [halves, halves, ((CHIPS, K, PAIRS_J), F32)],
        [],
        [coeffs, vectors],
        [],
        scratch=[
            pltpu.VMEM((CHUNKS - 1, CHUNK, PAIRS_L), F32),
            pltpu.VMEM((CHUNKS - 1, CHUNK, K), F32),
            pltpu.VMEM((TAIL, PAIRS_L), F32),
            pltpu.VMEM((TAIL, K), F32),
            pltpu.SemaphoreType.DMA((2, CHUNKS)),
        ],
        limit=26 << 20,
        us=8.0,
    )


def project_half(dev, bhi, blo, v, so_far, gram_rows=GRAM_J):
    def body(dev, bhi, blo, v, *rest):
        if so_far is None:
            acc, gacc = rest
            half = core_of(dev)
        else:
            acc0, gacc0, out, acc, gacc = rest
            half = 1 - core_of(dev)
        for i in range(3):
            row0 = pl.multiple_of(half * HALF + i * CHUNK, CHUNK)
            vt = transposed_halves(v[CHUNK * i : CHUNK * (i + 1), :])
            for n in range(4):
                part = fold(
                    dot(vt, bhi[n, pl.ds(row0, CHUNK), :], 1, 0)
                    + dot(vt, blo[n, pl.ds(row0, CHUNK), :], 1, 0)
                )
                for t in range(2):
                    value = part[:, 128 * t : 128 * t + 128]
                    j = 2 * n + t
                    if i > 0:
                        value = acc[j] + value
                    if so_far is not None and i == 2:
                        out[j, 0:K, :] = acc0[j] + value
                    else:
                        acc[j] = value
            g = dot(vt, vt, 1, 1)
            gacc[...] = g if i == 0 else gacc[...] + g
        if so_far is not None:
            g = gacc[...] + gacc0[...]
            gram = (g[0:K, 0:K] + g[K:, K:]) + (g[0:K, K:] + g[K:, 0:K])
            for j in range(CHIPS):
                first = GRAM_J * j if gram_rows < K else 0
                out[j, K:, :] = gram[first : first + gram_rows, :]

    acc = ((CHIPS, K, PAIRS_J), F32)
    gacc = ((2 * K, 2 * K), F32)
    if so_far is None:
        return kernel_call(body, [acc, gacc], [dev], [], [bhi, blo, v], us=3.0)
    return kernel_call(
        body,
        [((CHIPS, K + gram_rows, PAIRS_J), F32)],
        [dev],
        [],
        [bhi, blo, v, *so_far],
        scratch=[pltpu.VMEM(*acc), pltpu.VMEM(*gacc)],
        us=3.0,
    )


def sum_aux(dev, parts, gaps, copies):
    rows = parts.shape[1]

    def body(dev, p, gaps, *outs):
        gap = gaps[pl.ds(aux_of(dev), 1), :]
        s = ((p[0] + p[1]) + (p[2] + p[3])) + ((p[4] + p[5]) + (p[6] + p[7]))
        piece = s[0:K] * (4.0 * gap / (gap * gap + 1.0))
        if copies:
            for j in range(CHIPS):
                outs[0][j, 0:K, :] = piece
                if rows > K:
                    outs[0][j, K:, :] = s[K:]
        else:
            outs[0][...] = dot(piece, s[0:K], 1, 1, HIGHEST)
            outs[1][...] = s[K:]

    if copies:
        outs = [((CHIPS, rows, PAIRS_J), F32)]
    else:
        outs = [((K, K), F32), ((K, K), F32)]
    return kernel_call(body, outs, [dev], [], [parts, gaps])


NEAR_MASK = {("z", 1): 1, ("z", 3): 3, ("xl", 1): 4}
CROSS = ((("z", 1), ("z", 3), ("xl", 1)), (("xl", 1), ("z", 1), ("z", 3)))


def piece_at(core, near, p):
    masks = [0, 0]
    for c in range(2):
        for t in range(3):
            if (p >> (2 - t)) & 1:
                masks[c] ^= NEAR_MASK[CROSS[c][t]]
    return near ^ jnp.where(core == 0, masks[0], masks[1])


def apply_pieces(dev, bhi, blo, scaled, other, make_rhs, first):
    def body(dev, bhi, blo, s, out, *rest):
        if make_rhs:
            st = rest[0]
            for j in range(CHIPS):
                hi, lo = split(s[j, 0:K, :])
                lanes = slice(128 * (j % 2), 128 * (j % 2) + 128)
                st[j // 2, 0:K, lanes] = hi
                st[j // 2, K : 2 * K, lanes] = lo
        else:
            st = s
        core = core_of(dev)
        if other:
            core = 1 - core

        for i in range(4):
            start = core * HALF + piece_at(core, near_of(dev), first + i) * PIECE
            start = pl.multiple_of(start, PIECE)
            res = None
            for ref in (bhi, blo):
                for n in range(4):
                    d = dot(ref[n, pl.ds(start, PIECE), :], st[n], 1, 1)
                    res = d if res is None else res + d
            out[i] = res[:, 0:K] + res[:, K : 2 * K]

    outs = [((4, PIECE, K), F32)]
    if make_rhs:
        outs.append(((4, 2 * K, 256), BF16))
    return kernel_call(body, outs, [dev], [], [bhi, blo, scaled], us=1.4)


def add_slots(first, count, *parts):
    def body(*refs):
        total = refs[0][first : first + count]
        for r in refs[1:-1]:
            total = total + r[first : first + count]
        refs[-1][...] = total

    return kernel_call(body, [((count, PIECE, K), F32)], [], [], list(parts))[0]


def sum_rows(parts, inverse):
    def body(*refs):
        out = refs[-1]
        own, got, r1, r2, r3 = refs[:5]
        s = (own[0] + got[0]) + r1[0] + (r2[0] + r3[0])
        if inverse is not None:
            s = dot(s, refs[len(parts)][...], 1, 1, HIGHEST)
        for j in range(CHIPS):
            out[j] = s

    extra = [] if inverse is None else [inverse]
    return kernel_call(body, [((CHIPS, PIECE, K), F32)], [], [], [*parts, *extra])[0]


def pivots(gs, ws, begin, end):
    lane = lax.broadcasted_iota(jnp.int32, (K, K), 1)
    sub = lax.broadcasted_iota(jnp.int32, (K, K), 0)

    def step(h, low):
        k = 4 * h
        lanes, rows = lane[low:], sub[low:, 0:1]
        g, w_all = gs[low:, :], ws[low:, :]

        def pick(x, at):
            return jnp.sum(jnp.where(lanes[0 : x.shape[0]] == at, x, 0.0), axis=1, keepdims=True)

        r = [gs[pl.ds(k + i, 1), :] for i in range(4)]
        w = [ws[pl.ds(k + i, 1), :] for i in range(4)]
        c = [pick(g, k + i) for i in range(4)]
        d = [[pick(r[i], k + t) for t in range(4)] for i in range(4)]
        for i in range(4):
            inv = 1.0 / d[i][i]
            f = jnp.where(rows > k + i, c[i] * inv, 0.0)
            for t in range(i + 1, 4):
                c[t] = c[t] - f * d[i][t]
                m = d[t][i] * inv
                r[t] = r[t] - m * r[i]
                w[t] = w[t] - m * w[i]
                for u in range(i + 1, 4):
                    d[t][u] = d[t][u] - m * d[i][u]
            g = g - f * r[i]
            w_all = w_all - f * w[i]
        gs[low:, :] = g
        ws[low:, :] = w_all

    for low, top in ((0, 64), (64, K)):
        one, last = max(begin, low), min(end, top)
        if one < last:
            lax.fori_loop(one // 4, last // 4, lambda h, c, low=low: (step(h, low), c)[1], 0)


def scaled_rows(gs, ws):
    lane = lax.broadcasted_iota(jnp.int32, (K, K), 1)
    sub = lax.broadcasted_iota(jnp.int32, (K, K), 0)
    d = jnp.sum(jnp.where(lane == sub, gs[...], 0.0), axis=1, keepdims=True)
    return ws[...] / jnp.sqrt(d)


def eliminate(state, begin, end):
    start, stop = begin == 0, end == K

    def body(*refs):
        gs, ws = refs[-2:]
        if start:
            g_ref = refs[0]
            if len(g_ref.shape) == 2:
                gs[...] = g_ref[...]
            else:
                row0 = g_ref.shape[1] - GRAM_J
                for j in range(CHIPS):
                    gs[GRAM_J * j : GRAM_J * (j + 1), :] = g_ref[j, row0:, :]
            lane = lax.broadcasted_iota(jnp.int32, (K, K), 1)
            sub = lax.broadcasted_iota(jnp.int32, (K, K), 0)
            ws[...] = jnp.where(lane == sub, 1.0, 0.0).astype(F32)
        else:
            gs[...] = refs[0][...]
            ws[...] = refs[1][...]
        pivots(gs, ws, begin, end)
        if stop:
            refs[-3][...] = scaled_rows(gs, ws)

    square = ((K, K), F32)
    if stop:
        outs, scratch = [square], [pltpu.VMEM(*square), pltpu.VMEM(*square)]
    else:
        outs, scratch = [square, square], []
    return kernel_call(body, outs, [], [], list(state), scratch=scratch, us=(end - begin) / 20)


def in_between(value, state, cuts):
    state = eliminate(state, cuts[0], cuts[1])
    value, *state = lax.optimization_barrier((value, *state))
    return value, state


def finish(dev, mine, theirs, state, begin):
    def body(dev, mine, theirs, g, w, out, inv, gs, ws, both, buf, tail, sem):
        gs[...] = g[...]
        ws[...] = w[...]
        pivots(gs, ws, begin, K)
        inv[...] = scaled_rows(gs, ws)
        both[core_of(dev)] = mine[...]
        both[1 - core_of(dev)] = theirs[...]
        ihi, ilo = split(inv[...])
        rhs = jnp.concatenate([ihi, ilo], axis=0)

        def copy(i):
            last = i == CHUNKS - 1
            rows = pl.ds(i * CHUNK, TAIL if last else CHUNK)
            return pltpu.make_async_copy(tail if last else buf.at[i], out.at[rows], sem.at[i])

        for i in range(CHUNKS):
            start = CHUNK * (i % 3)
            vhi, vlo = split(both[i // 3, start : start + CHUNK, :])
            r = dot(vhi, rhs, 1, 1) + dot(vlo, rhs, 1, 1)
            r = r[:, 0:K] + r[:, K : 2 * K]
            if i == CHUNKS - 1:
                tail[...] = r[0:TAIL]
            else:
                buf[i] = r
            copy(i).start()
        for i in range(CHUNKS):
            copy(i).wait()

    square = pltpu.VMEM((K, K), F32)
    return pl.pallas_call(
        body,
        out_shape=[jax.ShapeDtypeStruct((NAUX_L, K), F32), square],
        in_specs=[pl.BlockSpec(memory_space=pltpu.SMEM)] + [VMEM_SPEC] * 4,
        out_specs=[pl.BlockSpec(memory_space=pl.ANY), VMEM_SPEC],
        scratch_shapes=[
            square,
            square,
            pltpu.VMEM((2, HALF, K), F32),
            pltpu.VMEM((CHUNKS - 1, CHUNK, K), F32),
            pltpu.VMEM((TAIL, K), F32),
            pltpu.SemaphoreType.DMA((CHUNKS,)),
        ],
        compiler_params=pltpu.CompilerParams(vmem_limit_bytes=16 << 20),
        cost_estimate=cost(4.2),
        name="finish",
    )(dev, *[pltpu.with_memory_space_constraint(v, pltpu.VMEM) for v in (mine, theirs, *state)])


def rayleigh_matrix(inverse, parts):
    def body(inv, a, b, c, d, out):
        total = (a[...] + b[...]) + (c[...] + d[...])
        out[...] = dot(dot(inv[...], total, 1, 0, HIGHEST), inv[...], 1, 1, HIGHEST)

    return kernel_call(body, [((K, K), F32)], [], [], [inverse, *parts])[0]


def exchange(value, axis, mask):
    n = lax.axis_size(axis)
    return lax.ppermute(value, axis, [(i, i ^ mask) for i in range(n)])


def to_each(value, axes):
    return lax.all_to_all(value, axes, split_axis=0, concat_axis=0, tiled=True)


NEAR = ("xl", "z")
AUX = ("xh", "y")


def cross(value, step):
    nz, nx = lax.axis_size("z"), lax.axis_size("xl")
    pairs = []
    for z in range(nz):
        for x in range(nx):
            for c in range(2):
                axis, mask = CROSS[c][step]
                to = (z ^ mask, x) if axis == "z" else (z, x ^ mask)
                pairs.append(((z * nx + x) * 2 + c, (to[0] * nx + to[1]) * 2 + c))
    return lax.ppermute(value, ("z", "xl", "c"), pairs)


def reduce_rows(dev, bhi, blo, scaled, eliminating):
    send, rhs = apply_pieces(dev, bhi, blo, scaled, True, True, 4)
    got = exchange(send, "c", 1)
    (own,) = apply_pieces(dev, bhi, blo, rhs, False, False, 4)
    first = add_slots(0, 4, own, got)
    r1 = cross(first, 0)
    first, rhs = lax.optimization_barrier((first, rhs))
    (send,) = apply_pieces(dev, bhi, blo, rhs, True, False, 0)
    got = exchange(send, "c", 1)
    (own,) = apply_pieces(dev, bhi, blo, rhs, False, False, 0)
    r1, own, got = lax.optimization_barrier((r1, own, got))
    inverse = None
    if eliminating:
        r1, state = in_between(r1, [scaled], (0, 40))
    r2 = cross(add_slots(2, 2, own, got, r1), 1)
    if eliminating:
        r2, state = in_between(r2, state, (40, 80))
    r3 = cross(add_slots(1, 1, own, got, r1, r2), 2)
    if eliminating:
        r3, (inverse,) = in_between(r3, state, (80, 128))
    return sum_rows([own, got, r1, r2, r3], inverse)


def shards(pair_coeffs, pair_gaps, trial_vectors):
    dev = lax.axis_index(("z", "xl", "c") + AUX).astype(jnp.int32)[None]
    gaps = pair_gaps.reshape(CHIPS, PAIRS_J)
    dev, gaps, trial_vectors = lax.optimization_barrier((dev, gaps, trial_vectors))
    bhi, blo, parts = first_projection(pair_coeffs, trial_vectors)
    for step in range(2):
        (copies,) = sum_aux(dev, to_each(parts, AUX), gaps, True)
        scaled = to_each(copies, AUX)
        near = reduce_rows(dev, bhi, blo, scaled, step == 1)
        mine = to_each(near, NEAR).reshape(HALF, K)
        theirs = exchange(mine, "c", 1)
        so_far = project_half(dev, bhi, blo, mine, None)
        (parts,) = project_half(dev, bhi, blo, theirs, so_far, K if step == 1 else GRAM_J)
    total, gram = sum_aux(dev, to_each(parts, AUX), gaps, False)
    total = total + exchange(total, "c", 1)
    state = [gram]
    for axis, cut in (("z", (0, 40)), ("y", (40, 84)), (("xl", "xh"), None)):
        got = []
        for mask in (1, 2, 3):
            got.append(exchange(total, axis, mask))
        if cut:
            got, state = in_between(got, state, cut)
            total = (total + got[0]) + (got[1] + got[2])
    vectors_out, inverse = finish(dev, mine, theirs, state, 84)
    rayleigh = rayleigh_matrix(inverse, [total, *got])
    return vectors_out, rayleigh


def solution(mesh):
    cube = Mesh(mesh.devices.reshape(4, 2, 2, 2, 4), ("z", "xl", "c", "xh", "y"))

    return jax.shard_map(
        shards,
        mesh=cube,
        in_specs=(P(AUX, ("z", "xl", "c")), P(("z", "xl", "c")), P(AUX, None)),
        out_specs=(P(AUX, None), P()),
        check_vma=False,
    )
```

```python
import itertools

import jax
import jax.numpy as jnp
from jax import lax
from jax.experimental import pallas as pl
from jax.experimental.pallas import tpu as pltpu
from jax.sharding import Mesh, PartitionSpec as P


F32 = jnp.float32
BF16 = jnp.bfloat16
HIGHEST = lax.Precision.HIGHEST

NAUX_L = 4500
PAIRS_L = 1024
K = 128
CHUNK = 768
CHUNKS = 6
ROWS = CHUNK * CHUNKS
HALF = ROWS // 2
TAIL = NAUX_L - CHUNK * (CHUNKS - 1)
CHIPS = 8
PIECE = HALF // CHIPS
PAIRS_J = PAIRS_L // CHIPS
GRAM_J = K // CHIPS


def split(x):
    hi = x.astype(BF16)
    return hi, (x - hi.astype(F32)).astype(BF16)


def dot(a, b, ca, cb, precision=None):
    return lax.dot_general(
        a, b, (((ca,), (cb,)), ((), ())), precision=precision, preferred_element_type=F32
    )


VMEM_SPEC = pl.BlockSpec(memory_space=pltpu.VMEM)


def cost(us):
    return pl.CostEstimate(flops=int(us * 1.5e8), bytes_accessed=0, transcendentals=0)


def core_of(dev):
    return (dev[0] >> 3) & 1


def near_of(dev):
    return ((dev[0] >> 4) & 1) * 4 + (dev[0] >> 5)


def aux_of(dev):
    return dev[0] & 7


def kernel_call(body, outs, smem, hbm, vmem, scratch=(), limit=12 << 20, us=0.3):
    return pl.pallas_call(
        body,
        out_shape=[pltpu.VMEM(s, d) for s, d in outs],
        in_specs=[pl.BlockSpec(memory_space=pltpu.SMEM)] * len(smem)
        + [pl.BlockSpec(memory_space=pl.ANY)] * len(hbm)
        + [VMEM_SPEC] * len(vmem),
        out_specs=[VMEM_SPEC] * len(outs),
        scratch_shapes=list(scratch),
        compiler_params=pltpu.CompilerParams(vmem_limit_bytes=limit),
        cost_estimate=cost(us),
    )(*smem, *hbm, *[pltpu.with_memory_space_constraint(v, pltpu.VMEM) for v in vmem])


MASK = {("z", 1): 1, ("z", 3): 3, ("xl", 1): 4, ("y", 1): 1, ("y", 3): 3, ("xh", 1): 4}
NEAR_LINKS = ((("z", 1), ("z", 3), ("xl", 1)), (("xl", 1), ("z", 1), ("z", 3)))
AUX_LINKS = ((("y", 1), ("y", 3), ("xh", 1)), (("y", 3), ("y", 1), ("xh", 1)))


def piece_at(links, core, me, p):
    masks = [0, 0]
    for c in range(2):
        for t in range(3):
            if (p >> (2 - t)) & 1:
                masks[c] ^= MASK[links[c][t]]
    return me ^ jnp.where(core == 0, masks[0], masks[1])


def transposed_halves(v):
    hi, lo = split(v.T)
    return jnp.concatenate([hi, lo], axis=0)


def fold(x):
    return x[0:K, :] + x[K : 2 * K, :]


def first_projection(coeffs, vectors):
    def body(b_hbm, v_hbm, bhi, blo, out, bbuf, vbuf, btail, vtail, sems):
        def copies(i):
            last = i == CHUNKS - 1
            rows = pl.ds(i * CHUNK, TAIL if last else CHUNK)
            return (
                pltpu.make_async_copy(b_hbm.at[rows], btail if last else bbuf.at[i], sems.at[0, i]),
                pltpu.make_async_copy(v_hbm.at[rows], vtail if last else vbuf.at[i], sems.at[1, i]),
            )

        for i in range(CHUNKS):
            for c in copies(i):
                c.start()

        def chunk(slot, row0, first):
            vt = transposed_halves(vbuf[slot])
            for n in range(4):
                hi, lo = split(bbuf[slot, :, 256 * n : 256 * n + 256])
                bhi[n, pl.ds(row0, CHUNK), :] = hi
                blo[n, pl.ds(row0, CHUNK), :] = lo
                part = fold(dot(vt, hi, 1, 0)) + dot(vt[0:K], lo, 1, 0)
                for t in range(2):
                    value = part[:, 128 * t : 128 * t + 128]
                    out[2 * n + t] = value if first else out[2 * n + t] + value

        for c in copies(0):
            c.wait()
        chunk(0, 0, True)

        def middle(i, carry):
            rows = pl.ds(pl.multiple_of(i * CHUNK, CHUNK), CHUNK)
            pltpu.make_async_copy(b_hbm.at[rows], bbuf.at[i], sems.at[0, i]).wait()
            pltpu.make_async_copy(v_hbm.at[rows], vbuf.at[i], sems.at[1, i]).wait()
            chunk(i, pl.multiple_of(i * CHUNK, CHUNK), False)
            return carry

        lax.fori_loop(1, CHUNKS - 1, middle, 0)
        for c in copies(CHUNKS - 1):
            c.wait()
        whole = TAIL // 8 * 8
        bbuf[0, whole:, :] = jnp.zeros((CHUNK - whole, PAIRS_L), F32)
        vbuf[0, whole:, :] = jnp.zeros((CHUNK - whole, K), F32)
        bbuf[0, 0:TAIL, :] = btail[...]
        vbuf[0, 0:TAIL, :] = vtail[...]
        chunk(0, CHUNK * (CHUNKS - 1), False)

    halves = ((4, ROWS, 256), BF16)
    coeffs = pltpu.with_memory_space_constraint(coeffs, pltpu.HBM)
    vectors = pltpu.with_memory_space_constraint(vectors, pltpu.HBM)
    return kernel_call(
        body,
        [halves, halves, ((CHIPS, K, PAIRS_J), F32)],
        [],
        [coeffs, vectors],
        [],
        scratch=[
            pltpu.VMEM((CHUNKS - 1, CHUNK, PAIRS_L), F32),
            pltpu.VMEM((CHUNKS - 1, CHUNK, K), F32),
            pltpu.VMEM((TAIL, PAIRS_L), F32),
            pltpu.VMEM((TAIL, K), F32),
            pltpu.SemaphoreType.DMA((2, CHUNKS)),
        ],
        limit=26 << 20,
        us=8.0,
    )


def project_half(dev, bhi, blo, v, so_far, by_position=False):
    def body(dev, bhi, blo, v, *rest):
        if so_far is None:
            acc, gacc = rest
            half = core_of(dev)
        else:
            acc0, gacc0, *outs, acc, gacc = rest
            half = 1 - core_of(dev)
        for i in range(3):
            row0 = pl.multiple_of(half * HALF + i * CHUNK, CHUNK)
            vt = transposed_halves(v[CHUNK * i : CHUNK * (i + 1), :])
            for n in range(4):
                part = fold(dot(vt, bhi[n, pl.ds(row0, CHUNK), :], 1, 0))
                part = part + dot(vt[0:K], blo[n, pl.ds(row0, CHUNK), :], 1, 0)
                for t in range(2):
                    value = part[:, 128 * t : 128 * t + 128]
                    j = 2 * n + t
                    if i > 0:
                        value = acc[j] + value
                    if so_far is not None and i == 2:
                        value = acc0[j] + value
                    acc[j] = value
            g = dot(vt, vt, 1, 1)
            gacc[...] = g if i == 0 else gacc[...] + g
        if so_far is not None:
            g = gacc[...] + gacc0[...]
            gram = (g[0:K, 0:K] + g[K:, K:]) + (g[0:K, K:] + g[K:, 0:K])
            if by_position:
                for t, out in enumerate(outs):
                    for p in range(4):
                        at = piece_at(AUX_LINKS, core_of(dev), aux_of(dev), 4 - 4 * t + p)
                        out[p] = acc[at]
                    out[4] = gram
            else:
                for j in range(CHIPS):
                    outs[0][j, 0:K, :] = acc[j]
                    outs[0][j, K:, :] = gram[GRAM_J * j : GRAM_J * (j + 1), :]

    acc = ((CHIPS, K, PAIRS_J), F32)
    gacc = ((2 * K, 2 * K), F32)
    if so_far is None:
        return kernel_call(body, [acc, gacc], [dev], [], [bhi, blo, v], us=3.0)
    return kernel_call(
        body,
        [((5, K, K), F32)] * 2 if by_position else [((CHIPS, K + GRAM_J, PAIRS_J), F32)],
        [dev],
        [],
        [bhi, blo, v, *so_far],
        scratch=[pltpu.VMEM(*acc), pltpu.VMEM(*gacc)],
        us=3.0,
    )


def weights_of(dev, gaps):
    gap = gaps[pl.ds(aux_of(dev), 1), :]
    return 4.0 * gap / (gap * gap + 1.0)


def sum_aux(dev, parts, gaps):
    def body(dev, p, gaps, out):
        s = ((p[0] + p[1]) + (p[2] + p[3])) + ((p[4] + p[5]) + (p[6] + p[7]))
        piece = s[0:K] * weights_of(dev, gaps)
        for j in range(CHIPS):
            out[j, 0:K, :] = piece
            if p.shape[1] > K:
                out[j, K:, :] = s[K:]

    return kernel_call(body, [(parts.shape, F32)], [dev], [], [parts, gaps])[0]


def reduce_aux(dev, send, keep, gaps):
    def last_step(k, r1, r2, out):
        out[0] = (k[1] + r1[1]) + r2[1]
        out[1] = (k[4] + r1[4]) + r2[2]

    def finish_sum(dev, k, r1, r2, r3, gaps, out):
        own = ((k[0] + r1[0]) + r2[0]) + r3[0]
        out[0] = dot(own * weights_of(dev, gaps), own, 1, 1, HIGHEST)
        out[1] = ((k[4] + r1[4]) + r2[2]) + r3[1]

    two = ((2, K, K), F32)
    r1 = cross(send, 0, AUX_LINKS)
    r2 = cross(add_slots(2, 3, keep, r1), 1, AUX_LINKS)
    (send,) = kernel_call(last_step, [two], [], [], [keep, r1, r2])
    r3 = cross(send, 2, AUX_LINKS)
    return kernel_call(finish_sum, [two], [dev], [], [keep, r1, r2, r3, gaps])[0]


def add_over_cores(dev, both):
    def body(dev, own, got, total, gram):
        total[...] = own[0] + got[0]
        gram[...] = jnp.where(core_of(dev) == 1, own[1], got[1])

    got = exchange(both, "c", 1)
    return kernel_call(body, [((K, K), F32)] * 2, [dev], [], [both, got])


def apply_pieces(dev, bhi, blo, scaled, other, make_rhs, first):
    def body(dev, bhi, blo, s, out, *rest):
        if make_rhs:
            st = rest[0]
            for j in range(CHIPS):
                hi, lo = split(s[j, 0:K, :])
                lanes = slice(128 * (j % 2), 128 * (j % 2) + 128)
                st[j // 2, 0:K, lanes] = hi
                st[j // 2, K : 2 * K, lanes] = lo
        else:
            st = s
        core = core_of(dev)
        if other:
            core = 1 - core

        for i in range(2):
            start = core * HALF + piece_at(NEAR_LINKS, core, near_of(dev), first + i) * PIECE
            start = pl.multiple_of(start, PIECE)
            res = None
            for ref in (bhi, blo):
                for n in range(4):
                    d = dot(ref[n, pl.ds(start, PIECE), :], st[n], 1, 1)
                    res = d if res is None else res + d
            out[i] = res[:, 0:K] + res[:, K : 2 * K]

    outs = [((2, PIECE, K), F32)]
    if make_rhs:
        outs.append(((4, 2 * K, 256), BF16))
    return kernel_call(body, outs, [dev], [], [bhi, blo, scaled], us=0.75)


def add_slots(first, count, *parts):
    def body(*refs):
        total = refs[0][first : first + count]
        for r in refs[1:-1]:
            total = total + r[first : first + count]
        refs[-1][...] = total

    shape = (count, *parts[0].shape[1:])
    return kernel_call(body, [(shape, F32)], [], [], list(parts))[0]


def sum_rows(parts, inverse):
    def body(*refs):
        out = refs[-1]
        own, got, r1, r2, r3 = refs[:5]
        s = ((own[0] + got[0]) + r1[0]) + (r2[0] + r3[0])
        if inverse is not None:
            s = dot(s, refs[len(parts)][...], 1, 1, HIGHEST)
        out[0] = s

    extra = [] if inverse is None else [inverse]
    return kernel_call(body, [((1, PIECE, K), F32)], [], [], [*parts, *extra])[0]


def pivots(gs, ws, begin, end):
    lane = lax.broadcasted_iota(jnp.int32, (K, K), 1)
    sub = lax.broadcasted_iota(jnp.int32, (K, K), 0)

    def step(h, low):
        k = 4 * h
        lanes, rows = lane[low:], sub[low:, 0:1]
        g, w_all = gs[low:, :], ws[low:, :]

        def pick(x, at):
            return jnp.sum(jnp.where(lanes[0 : x.shape[0]] == at, x, 0.0), axis=1, keepdims=True)

        r = [gs[pl.ds(k + i, 1), :] for i in range(4)]
        w = [ws[pl.ds(k + i, 1), :] for i in range(4)]
        c = [pick(g, k + i) for i in range(4)]
        d = [[pick(r[i], k + t) for t in range(4)] for i in range(4)]
        for i in range(4):
            inv = 1.0 / d[i][i]
            f = jnp.where(rows > k + i, c[i] * inv, 0.0)
            for t in range(i + 1, 4):
                c[t] = c[t] - f * d[i][t]
                m = d[t][i] * inv
                r[t] = r[t] - m * r[i]
                w[t] = w[t] - m * w[i]
                for u in range(i + 1, 4):
                    d[t][u] = d[t][u] - m * d[i][u]
            g = g - f * r[i]
            w_all = w_all - f * w[i]
        gs[low:, :] = g
        ws[low:, :] = w_all

    for low, top in ((0, 64), (64, K)):
        one, last = max(begin, low), min(end, top)
        if one < last:
            lax.fori_loop(one // 4, last // 4, lambda h, c, low=low: (step(h, low), c)[1], 0)


def scaled_rows(gs, ws):
    lane = lax.broadcasted_iota(jnp.int32, (K, K), 1)
    sub = lax.broadcasted_iota(jnp.int32, (K, K), 0)
    d = jnp.sum(jnp.where(lane == sub, gs[...], 0.0), axis=1, keepdims=True)
    return ws[...] / jnp.sqrt(d)


def eliminate(state, begin, end):
    start, stop = begin == 0, end == K

    def body(*refs):
        gs, ws = refs[-2:]
        if start:
            g_ref = refs[0]
            if len(g_ref.shape) == 2:
                gs[...] = g_ref[...]
            else:
                row0 = g_ref.shape[1] - GRAM_J
                for j in range(CHIPS):
                    gs[GRAM_J * j : GRAM_J * (j + 1), :] = g_ref[j, row0:, :]
            lane = lax.broadcasted_iota(jnp.int32, (K, K), 1)
            sub = lax.broadcasted_iota(jnp.int32, (K, K), 0)
            ws[...] = jnp.where(lane == sub, 1.0, 0.0).astype(F32)
        else:
            gs[...] = refs[0][...]
            ws[...] = refs[1][...]
        pivots(gs, ws, begin, end)
        if stop:
            refs[-3][...] = scaled_rows(gs, ws)

    square = ((K, K), F32)
    if stop:
        outs, scratch = [square], [pltpu.VMEM(*square), pltpu.VMEM(*square)]
    else:
        outs, scratch = [square, square], []
    return kernel_call(body, outs, [], [], list(state), scratch=scratch, us=(end - begin) / 20)


def in_between(value, state, cuts):
    state = eliminate(state, cuts[0], cuts[1])
    value, *state = lax.optimization_barrier((value, *state))
    return value, state


def finish(dev, mine, theirs, state, begin):
    def body(dev, mine, theirs, g, w, out, inv, gs, ws, both, buf, tail, sem):
        gs[...] = g[...]
        ws[...] = w[...]
        pivots(gs, ws, begin, K)
        inv[...] = scaled_rows(gs, ws)
        both[core_of(dev)] = mine[...]
        both[1 - core_of(dev)] = theirs[...]
        ihi, ilo = split(inv[...])
        rhs = jnp.concatenate([ihi, ilo], axis=0)

        def copy(i):
            last = i == CHUNKS - 1
            rows = pl.ds(i * CHUNK, TAIL if last else CHUNK)
            return pltpu.make_async_copy(tail if last else buf.at[i], out.at[rows], sem.at[i])

        for i in range(CHUNKS):
            start = CHUNK * (i % 3)
            vhi, vlo = split(both[i // 3, start : start + CHUNK, :])
            r = dot(vhi, rhs, 1, 1) + dot(vlo, rhs, 1, 1)
            r = r[:, 0:K] + r[:, K : 2 * K]
            if i == CHUNKS - 1:
                tail[...] = r[0:TAIL]
            else:
                buf[i] = r
            copy(i).start()
        for i in range(CHUNKS):
            copy(i).wait()

    square = pltpu.VMEM((K, K), F32)
    return pl.pallas_call(
        body,
        out_shape=[jax.ShapeDtypeStruct((NAUX_L, K), F32), square],
        in_specs=[pl.BlockSpec(memory_space=pltpu.SMEM)] + [VMEM_SPEC] * 4,
        out_specs=[pl.BlockSpec(memory_space=pl.ANY), VMEM_SPEC],
        scratch_shapes=[
            square,
            square,
            pltpu.VMEM((2, HALF, K), F32),
            pltpu.VMEM((CHUNKS - 1, CHUNK, K), F32),
            pltpu.VMEM((TAIL, K), F32),
            pltpu.SemaphoreType.DMA((CHUNKS,)),
        ],
        compiler_params=pltpu.CompilerParams(vmem_limit_bytes=16 << 20),
        cost_estimate=cost(4.2),
        name="finish",
    )(dev, *[pltpu.with_memory_space_constraint(v, pltpu.VMEM) for v in (mine, theirs, *state)])


def rayleigh_matrix(inverse, parts):
    def body(inv, a, b, c, d, out):
        total = (a[...] + b[...]) + (c[...] + d[...])
        out[...] = dot(dot(inv[...], total, 1, 0, HIGHEST), inv[...], 1, 1, HIGHEST)

    return kernel_call(body, [((K, K), F32)], [], [], [inverse, *parts])[0]


def exchange(value, axis, mask):
    n = lax.axis_size(axis)
    return lax.ppermute(value, axis, [(i, i ^ mask) for i in range(n)])


def to_each(value, axes):
    return lax.all_to_all(value, axes, split_axis=0, concat_axis=0, tiled=True)


AUX = ("xh", "y")


def cross(value, step, links=NEAR_LINKS):
    axes = ("z", "xl", "c") if links is NEAR_LINKS else ("c", "xh", "y")
    sizes = [lax.axis_size(a) for a in axes]
    pairs = []
    for at in itertools.product(*map(range, sizes)):
        to = dict(zip(axes, at))
        axis, mask = links[to["c"]][step]
        to[axis] ^= mask
        ids = [(a * sizes[1] + b) * sizes[2] + c for a, b, c in (at, tuple(to.values()))]
        pairs.append(tuple(ids))
    return lax.ppermute(value, axes, pairs)


def reduce_rows(dev, bhi, blo, scaled, eliminating):
    rhs = None

    def apply_pair(first):
        nonlocal rhs
        send, *made = apply_pieces(
            dev, bhi, blo, scaled if rhs is None else rhs, True, rhs is None, first
        )
        rhs = made[0] if made else rhs
        got = exchange(send, "c", 1)
        (own,) = apply_pieces(dev, bhi, blo, rhs, False, False, first)
        return own, got

    steps = []
    for first in (6, 4, 2, 0):
        own, got = apply_pair(first)
        if first == 0:
            break
        value = add_slots(0, 2, own, got, *(steps[:1] if first == 2 else ()))
        steps.append(cross(value, 1 if first == 2 else 0))
        value, rhs = lax.optimization_barrier((value, rhs))
    _, r1, r2 = steps
    inverse = None
    if eliminating:
        r2, own, got = lax.optimization_barrier((r2, own, got))
        r2, state = in_between(r2, [scaled], (0, 64))
    r3 = cross(add_slots(1, 1, own, got, r1, r2), 2)
    if eliminating:
        r3, (inverse,) = in_between(r3, state, (64, 128))
    return sum_rows([own, got, r1, r2, r3], inverse)


def gather_rows(dev, own):
    p = [own] + [None] * 7
    for a, step in ((0, 2), (0, 1), (0, 0), (1, 1), (1, 0), (2, 0), (3, 0)):
        at = a | (4 >> step)
        p[at] = cross(p[a], step)

    def body(dev, *refs):
        for at in range(CHIPS):
            to = piece_at(NEAR_LINKS, core_of(dev), near_of(dev), at)
            refs[-1][to] = refs[at][0]

    pieces = ((CHIPS, PIECE, K), F32)
    return kernel_call(body, [pieces], [dev], [], p)[0].reshape(HALF, K)


def shards(pair_coeffs, pair_gaps, trial_vectors):
    dev = lax.axis_index(("z", "xl", "c") + AUX).astype(jnp.int32)[None]
    gaps = pair_gaps.reshape(CHIPS, PAIRS_J)
    dev, gaps, trial_vectors = lax.optimization_barrier((dev, gaps, trial_vectors))
    bhi, blo, parts = first_projection(pair_coeffs, trial_vectors)
    for step in range(2):
        scaled = to_each(sum_aux(dev, to_each(parts, AUX), gaps), AUX)
        mine = gather_rows(dev, reduce_rows(dev, bhi, blo, scaled, step == 1))
        theirs = exchange(mine, "c", 1)
        so_far = project_half(dev, bhi, blo, mine, None)
        parts, *kept = project_half(dev, bhi, blo, theirs, so_far, step == 1)
    total, gram = add_over_cores(dev, reduce_aux(dev, parts, *kept, gaps))
    state = [gram]
    for axis, cut in (("z", (0, 40)), ("y", (40, 84)), (("xl", "xh"), None)):
        got = []
        for mask in (1, 2, 3):
            got.append(exchange(total, axis, mask))
        if cut:
            got, state = in_between(got, state, cut)
            total = (total + got[0]) + (got[1] + got[2])
    vectors_out, inverse = finish(dev, mine, theirs, state, 84)
    rayleigh = rayleigh_matrix(inverse, [total, *got])
    return vectors_out, rayleigh


def solution(mesh):
    cube = Mesh(mesh.devices.reshape(4, 2, 2, 2, 4), ("z", "xl", "c", "xh", "y"))

    return jax.shard_map(
        shards,
        mesh=cube,
        in_specs=(P(AUX, ("z", "xl", "c")), P(("z", "xl", "c")), P(AUX, None)),
        out_specs=(P(AUX, None), P()),
        check_vma=False,
    )
```

```python
import itertools

import jax
import jax.numpy as jnp
from jax import lax
from jax.experimental import pallas as pl
from jax.experimental.pallas import tpu as pltpu
from jax.sharding import Mesh, PartitionSpec as P


F32 = jnp.float32
BF16 = jnp.bfloat16
HIGHEST = lax.Precision.HIGHEST

NAUX_L = 4500
PAIRS_L = 1024
K = 128
CHUNK = 768
CHUNKS = 6
ROWS = CHUNK * CHUNKS
HALF = ROWS // 2
TAIL = NAUX_L - CHUNK * (CHUNKS - 1)
CHIPS = 8
PIECE = HALF // CHIPS
PAIRS_J = PAIRS_L // CHIPS
GRAM_J = K // CHIPS


def split(x):
    hi = x.astype(BF16)
    return hi, (x - hi.astype(F32)).astype(BF16)


def dot(a, b, ca, cb, precision=None):
    return lax.dot_general(
        a, b, (((ca,), (cb,)), ((), ())), precision=precision, preferred_element_type=F32
    )


VMEM_SPEC = pl.BlockSpec(memory_space=pltpu.VMEM)


def cost(us):
    return pl.CostEstimate(flops=int(us * 1.5e8), bytes_accessed=0, transcendentals=0)


def core_of(dev):
    return (dev[0] >> 3) & 1


def near_of(dev):
    return ((dev[0] >> 4) & 1) * 4 + (dev[0] >> 5)


def aux_of(dev):
    return dev[0] & 7


def kernel_call(body, outs, smem, hbm, vmem, scratch=(), limit=12 << 20, us=0.3):
    return pl.pallas_call(
        body,
        out_shape=[pltpu.VMEM(s, d) for s, d in outs],
        in_specs=[pl.BlockSpec(memory_space=pltpu.SMEM)] * len(smem)
        + [pl.BlockSpec(memory_space=pl.ANY)] * len(hbm)
        + [VMEM_SPEC] * len(vmem),
        out_specs=[VMEM_SPEC] * len(outs),
        scratch_shapes=list(scratch),
        compiler_params=pltpu.CompilerParams(vmem_limit_bytes=limit),
        cost_estimate=cost(us),
    )(*smem, *hbm, *[pltpu.with_memory_space_constraint(v, pltpu.VMEM) for v in vmem])


MASK = {("z", 1): 1, ("z", 3): 3, ("xl", 1): 4, ("y", 1): 1, ("y", 3): 3, ("xh", 1): 4}
NEAR_LINKS = ((("z", 1), ("z", 3), ("xl", 1)), (("xl", 1), ("z", 1), ("z", 3)))
AUX_LINKS = ((("y", 1), ("y", 3), ("xh", 1)), (("y", 3), ("y", 1), ("xh", 1)))


def piece_at(links, core, me, p):
    masks = [0, 0]
    for c in range(2):
        for t in range(3):
            if (p >> (2 - t)) & 1:
                masks[c] ^= MASK[links[c][t]]
    return me ^ jnp.where(core == 0, masks[0], masks[1])


def transposed_halves(v):
    hi, lo = split(v.T)
    return jnp.concatenate([hi, lo], axis=0)


def fold(x):
    return x[0:K, :] + x[K : 2 * K, :]


def first_projection(coeffs, vectors):
    def body(b_hbm, v_hbm, bhi, blo, out, bbuf, vbuf, btail, vtail, sems):
        def copies(i):
            last = i == CHUNKS - 1
            rows = pl.ds(i * CHUNK, TAIL if last else CHUNK)
            return (
                pltpu.make_async_copy(b_hbm.at[rows], btail if last else bbuf.at[i], sems.at[0, i]),
                pltpu.make_async_copy(v_hbm.at[rows], vtail if last else vbuf.at[i], sems.at[1, i]),
            )

        for i in range(CHUNKS):
            for c in copies(i):
                c.start()

        def chunk(slot, row0):
            vt = transposed_halves(vbuf[slot])
            for n in range(4):
                hi, lo = split(bbuf[slot, :, 256 * n : 256 * n + 256])
                bhi[n, pl.ds(row0, CHUNK), :] = hi
                blo[n, pl.ds(row0, CHUNK), :] = lo
                part = fold(dot(vt, hi, 1, 0)) + dot(vt[0:K], lo, 1, 0)
                for t in range(2):
                    out[2 * n + t] += part[:, 128 * t : 128 * t + 128]

        out[...] = jnp.zeros(out.shape, F32)

        def middle(i, carry):
            rows = pl.ds(pl.multiple_of(i * CHUNK, CHUNK), CHUNK)
            pltpu.make_async_copy(b_hbm.at[rows], bbuf.at[i], sems.at[0, i]).wait()
            pltpu.make_async_copy(v_hbm.at[rows], vbuf.at[i], sems.at[1, i]).wait()
            chunk(i, pl.multiple_of(i * CHUNK, CHUNK))
            return carry

        lax.fori_loop(0, CHUNKS - 1, middle, 0)
        for c in copies(CHUNKS - 1):
            c.wait()
        whole = TAIL // 8 * 8
        bbuf[0, whole:, :] = jnp.zeros((CHUNK - whole, PAIRS_L), F32)
        vbuf[0, whole:, :] = jnp.zeros((CHUNK - whole, K), F32)
        bbuf[0, 0:TAIL, :] = btail[...]
        vbuf[0, 0:TAIL, :] = vtail[...]
        chunk(0, CHUNK * (CHUNKS - 1))

    halves = ((4, ROWS, 256), BF16)
    coeffs = pltpu.with_memory_space_constraint(coeffs, pltpu.HBM)
    vectors = pltpu.with_memory_space_constraint(vectors, pltpu.HBM)
    return kernel_call(
        body,
        [halves, halves, ((CHIPS, K, PAIRS_J), F32)],
        [],
        [coeffs, vectors],
        [],
        scratch=[
            pltpu.VMEM((CHUNKS - 1, CHUNK, PAIRS_L), F32),
            pltpu.VMEM((CHUNKS - 1, CHUNK, K), F32),
            pltpu.VMEM((TAIL, PAIRS_L), F32),
            pltpu.VMEM((TAIL, K), F32),
            pltpu.SemaphoreType.DMA((2, CHUNKS)),
        ],
        limit=26 << 20,
        us=8.0,
    )


def project_half(dev, bhi, blo, v, so_far, by_position=False):
    def body(dev, bhi, blo, v, *rest):
        if so_far is None:
            acc, gacc = rest
            half = core_of(dev)
        else:
            acc0, gacc0, *outs, acc, gacc = rest
            half = 1 - core_of(dev)
        for i in range(3):
            row0 = pl.multiple_of(half * HALF + i * CHUNK, CHUNK)
            vt = transposed_halves(v[CHUNK * i : CHUNK * (i + 1), :])
            for n in range(4):
                part = fold(dot(vt, bhi[n, pl.ds(row0, CHUNK), :], 1, 0))
                part = part + dot(vt[0:K], blo[n, pl.ds(row0, CHUNK), :], 1, 0)
                for t in range(2):
                    value = part[:, 128 * t : 128 * t + 128]
                    j = 2 * n + t
                    if i > 0:
                        value = acc[j] + value
                    if so_far is not None and i == 2:
                        value = acc0[j] + value
                    acc[j] = value
            g = dot(vt, vt, 1, 1)
            gacc[...] = g if i == 0 else gacc[...] + g
        if so_far is not None:
            g = gacc[...] + gacc0[...]
            gram = (g[0:K, 0:K] + g[K:, K:]) + (g[0:K, K:] + g[K:, 0:K])
            if by_position:
                for out, places in zip(outs, ((6, 7), (4, 5), (0, 1, 2, 3))):
                    for t, p in enumerate(places):
                        out[t] = acc[piece_at(AUX_LINKS, core_of(dev), aux_of(dev), p)]
                outs[0][2] = gram
                outs[2][4] = gram
            else:
                for j in range(CHIPS):
                    outs[0][j, 0:K, :] = acc[j]
                    outs[0][j, K:, :] = gram[GRAM_J * j : GRAM_J * (j + 1), :]

    acc = ((CHIPS, K, PAIRS_J), F32)
    gacc = ((2 * K, 2 * K), F32)
    if so_far is None:
        return kernel_call(body, [acc, gacc], [dev], [], [bhi, blo, v], us=3.0)
    return kernel_call(
        body,
        [((n, K, K), F32) for n in (3, 2, 5)]
        if by_position
        else [((CHIPS, K + GRAM_J, PAIRS_J), F32)],
        [dev],
        [],
        [bhi, blo, v, *so_far],
        scratch=[pltpu.VMEM(*acc), pltpu.VMEM(*gacc)],
        us=3.0,
    )


def weights_of(dev, gaps):
    gap = gaps[pl.ds(aux_of(dev), 1), :]
    return 4.0 * gap / (gap * gap + 1.0)


def sum_aux(dev, parts, gaps):
    def body(dev, p, gaps, out):
        s = ((p[0] + p[1]) + (p[2] + p[3])) + ((p[4] + p[5]) + (p[6] + p[7]))
        piece = s[0:K] * weights_of(dev, gaps)
        for j in range(CHIPS):
            out[j, 0:K, :] = piece
            if p.shape[1] > K:
                out[j, K:, :] = s[K:]

    return kernel_call(body, [(parts.shape, F32)], [dev], [], [parts, gaps])[0]


def reduce_aux(dev, early, late, keep, gaps):
    def last_step(k, ra, rb, r2, out):
        out[0] = (k[1] + rb[1]) + r2[1]
        out[1] = (k[4] + ra[2]) + r2[2]

    def finish_sum(dev, k, ra, rb, r2, r3, gaps, out):
        own = ((k[0] + rb[0]) + r2[0]) + r3[0]
        out[0] = dot(own * weights_of(dev, gaps), own, 1, 1, HIGHEST)
        out[1] = ((k[4] + ra[2]) + r2[2]) + r3[1]

    def second_step(k, ra, out):
        out[...] = k[2:5] + ra[...]

    def pieces(n):
        return [((n, K, K), F32)]

    ra = cross(early, 0, AUX_LINKS)
    rb = cross(late, 0, AUX_LINKS)
    (send,) = kernel_call(second_step, pieces(3), [], [], [keep, ra])
    r2 = cross(send, 1, AUX_LINKS)
    (send,) = kernel_call(last_step, pieces(2), [], [], [keep, ra, rb, r2])
    r3 = cross(send, 2, AUX_LINKS)
    return kernel_call(finish_sum, pieces(2), [dev], [], [keep, ra, rb, r2, r3, gaps])[0]


def add_over_cores(dev, both):
    def body(dev, own, got, total, gram):
        total[...] = own[0] + got[0]
        gram[...] = jnp.where(core_of(dev) == 1, own[1], got[1])

    got = exchange(both, "c", 1)
    return kernel_call(body, [((K, K), F32)] * 2, [dev], [], [both, got])


def apply_pieces(dev, bhi, blo, scaled, other, make_rhs, first):
    def body(dev, bhi, blo, s, out, *rest):
        if make_rhs:
            st = rest[0]
            for j in range(CHIPS):
                hi, lo = split(s[j, 0:K, :])
                lanes = slice(128 * (j % 2), 128 * (j % 2) + 128)
                st[j // 2, 0:K, lanes] = hi
                st[j // 2, K : 2 * K, lanes] = lo
        else:
            st = s
        core = core_of(dev)
        if other:
            core = 1 - core

        for i in range(2):
            start = core * HALF + piece_at(NEAR_LINKS, core, near_of(dev), first + i) * PIECE
            start = pl.multiple_of(start, PIECE)
            res = None
            for ref in (bhi, blo):
                for n in range(4):
                    d = dot(ref[n, pl.ds(start, PIECE), :], st[n], 1, 1)
                    res = d if res is None else res + d
            out[i] = res[:, 0:K] + res[:, K : 2 * K]

    outs = [((2, PIECE, K), F32)]
    if make_rhs:
        outs.append(((4, 2 * K, 256), BF16))
    return kernel_call(body, outs, [dev], [], [bhi, blo, scaled], us=0.75)


def add_slots(first, count, *parts):
    def body(*refs):
        total = refs[0][first : first + count]
        for r in refs[1:-1]:
            total = total + r[first : first + count]
        refs[-1][...] = total

    shape = (count, *parts[0].shape[1:])
    return kernel_call(body, [(shape, F32)], [], [], list(parts))[0]


def add_last(own, got, r1, r2):
    def body(own, got, r1, r2, out):
        out[0] = ((own[1] + got[1]) + r1[1]) + r2[0]

    return kernel_call(body, [((1, PIECE, K), F32)], [], [], [own, got, r1, r2])[0]


def sum_rows(parts, inverse):
    def body(*refs):
        out = refs[-1]
        own, got, r1, r2, r3 = refs[:5]
        s = ((own[0] + got[0]) + r1[0]) + (r2[0] + r3[0])
        if inverse is not None:
            s = dot(s, refs[len(parts)][...], 1, 1, HIGHEST)
        out[0] = s

    extra = [] if inverse is None else [inverse]
    return kernel_call(body, [((1, PIECE, K), F32)], [], [], [*parts, *extra])[0]


def pivots(gs, ws, begin, end):
    lane = lax.broadcasted_iota(jnp.int32, (K, K), 1)
    sub = lax.broadcasted_iota(jnp.int32, (K, K), 0)

    def step(h, low):
        k = 4 * h
        lanes, rows = lane[low:], sub[low:, 0:1]
        g, w_all = gs[low:, :], ws[low:, :]

        def pick(x, at):
            return jnp.sum(jnp.where(lanes[0 : x.shape[0]] == at, x, 0.0), axis=1, keepdims=True)

        r = [gs[pl.ds(k + i, 1), :] for i in range(4)]
        w = [ws[pl.ds(k + i, 1), :] for i in range(4)]
        c = [pick(g, k + i) for i in range(4)]
        d = [[pick(r[i], k + t) for t in range(4)] for i in range(4)]
        for i in range(4):
            inv = 1.0 / d[i][i]
            f = jnp.where(rows > k + i, c[i] * inv, 0.0)
            for t in range(i + 1, 4):
                c[t] = c[t] - f * d[i][t]
                m = d[t][i] * inv
                r[t] = r[t] - m * r[i]
                w[t] = w[t] - m * w[i]
                for u in range(i + 1, 4):
                    d[t][u] = d[t][u] - m * d[i][u]
            g = g - f * r[i]
            w_all = w_all - f * w[i]
        gs[low:, :] = g
        ws[low:, :] = w_all

    for low, top in ((0, 64), (64, K)):
        one, last = max(begin, low), min(end, top)
        if one < last:
            lax.fori_loop(one // 4, last // 4, lambda h, c, low=low: (step(h, low), c)[1], 0)


def scaled_rows(gs, ws):
    lane = lax.broadcasted_iota(jnp.int32, (K, K), 1)
    sub = lax.broadcasted_iota(jnp.int32, (K, K), 0)
    d = jnp.sum(jnp.where(lane == sub, gs[...], 0.0), axis=1, keepdims=True)
    return ws[...] / jnp.sqrt(d)


def eliminate(state, begin, end):
    start, stop = begin == 0, end == K

    def body(*refs):
        gs, ws = refs[-2:]
        if start:
            g_ref = refs[0]
            if len(g_ref.shape) == 2:
                gs[...] = g_ref[...]
            else:
                row0 = g_ref.shape[1] - GRAM_J
                for j in range(CHIPS):
                    gs[GRAM_J * j : GRAM_J * (j + 1), :] = g_ref[j, row0:, :]
            lane = lax.broadcasted_iota(jnp.int32, (K, K), 1)
            sub = lax.broadcasted_iota(jnp.int32, (K, K), 0)
            ws[...] = jnp.where(lane == sub, 1.0, 0.0).astype(F32)
        else:
            gs[...] = refs[0][...]
            ws[...] = refs[1][...]
        pivots(gs, ws, begin, end)
        if stop:
            refs[-3][...] = scaled_rows(gs, ws)

    square = ((K, K), F32)
    if stop:
        outs, scratch = [square], [pltpu.VMEM(*square), pltpu.VMEM(*square)]
    else:
        outs, scratch = [square, square], []
    return kernel_call(body, outs, [], [], list(state), scratch=scratch, us=(end - begin) / 20)


def in_between(value, state, cuts):
    state = eliminate(state, cuts[0], cuts[1])
    value, *state = lax.optimization_barrier((value, *state))
    return value, state


def finish(dev, mine, theirs, state, begin):
    def body(dev, mine, theirs, g, w, out, inv, gs, ws, both, buf, tail, sem):
        gs[...] = g[...]
        ws[...] = w[...]
        pivots(gs, ws, begin, K)
        inv[...] = scaled_rows(gs, ws)
        both[core_of(dev)] = mine[...]
        both[1 - core_of(dev)] = theirs[...]
        ihi, ilo = split(inv[...])
        rhs = jnp.concatenate([ihi, ilo], axis=0)

        def copy(i):
            last = i == CHUNKS - 1
            rows = pl.ds(i * CHUNK, TAIL if last else CHUNK)
            return pltpu.make_async_copy(tail if last else buf.at[i], out.at[rows], sem.at[i])

        for i in range(CHUNKS):
            start = CHUNK * (i % 3)
            vhi, vlo = split(both[i // 3, start : start + CHUNK, :])
            r = dot(vhi, rhs, 1, 1) + dot(vlo, rhs, 1, 1)
            r = r[:, 0:K] + r[:, K : 2 * K]
            if i == CHUNKS - 1:
                tail[...] = r[0:TAIL]
            else:
                buf[i] = r
            copy(i).start()
        for i in range(CHUNKS):
            copy(i).wait()

    square = pltpu.VMEM((K, K), F32)
    return pl.pallas_call(
        body,
        out_shape=[jax.ShapeDtypeStruct((NAUX_L, K), F32), square],
        in_specs=[pl.BlockSpec(memory_space=pltpu.SMEM)] + [VMEM_SPEC] * 4,
        out_specs=[pl.BlockSpec(memory_space=pl.ANY), VMEM_SPEC],
        scratch_shapes=[
            square,
            square,
            pltpu.VMEM((2, HALF, K), F32),
            pltpu.VMEM((CHUNKS - 1, CHUNK, K), F32),
            pltpu.VMEM((TAIL, K), F32),
            pltpu.SemaphoreType.DMA((CHUNKS,)),
        ],
        compiler_params=pltpu.CompilerParams(vmem_limit_bytes=16 << 20),
        cost_estimate=cost(4.2),
        name="finish",
    )(dev, *[pltpu.with_memory_space_constraint(v, pltpu.VMEM) for v in (mine, theirs, *state)])


def rayleigh_matrix(inverse, parts):
    def body(inv, a, b, c, d, out):
        total = (a[...] + b[...]) + (c[...] + d[...])
        out[...] = dot(dot(inv[...], total, 1, 0, HIGHEST), inv[...], 1, 1, HIGHEST)

    return kernel_call(body, [((K, K), F32)], [], [], [inverse, *parts])[0]


def exchange(value, axis, mask):
    n = lax.axis_size(axis)
    return lax.ppermute(value, axis, [(i, i ^ mask) for i in range(n)])


def to_each(value, axes):
    return lax.all_to_all(value, axes, split_axis=0, concat_axis=0, tiled=True)


AUX = ("xh", "y")


def cross(value, step, links=NEAR_LINKS):
    axes = ("z", "xl", "c") if links is NEAR_LINKS else ("c", "xh", "y")
    sizes = [lax.axis_size(a) for a in axes]
    pairs = []
    for at in itertools.product(*map(range, sizes)):
        to = dict(zip(axes, at))
        axis, mask = links[to["c"]][step]
        to[axis] ^= mask
        ids = [(a * sizes[1] + b) * sizes[2] + c for a, b, c in (at, tuple(to.values()))]
        pairs.append(tuple(ids))
    return lax.ppermute(value, axes, pairs)


def reduce_rows(dev, bhi, blo, scaled, eliminating):
    rhs = None

    def apply_pair(first):
        nonlocal rhs
        send, *made = apply_pieces(
            dev, bhi, blo, scaled if rhs is None else rhs, True, rhs is None, first
        )
        rhs = made[0] if made else rhs
        got = exchange(send, "c", 1)
        (own,) = apply_pieces(dev, bhi, blo, rhs, False, False, first)
        return own, got

    steps = []
    for first in (6, 4, 2, 0):
        own, got = apply_pair(first)
        if first == 0:
            break
        if first > 2:
            value = add_slots(0, 2, own, got)
            steps.append(cross(value, 0))
        else:
            for slot in (1, 0):
                value = add_slots(slot, 1, own, got, steps[0])
                steps.append(cross(value, 1))
        value, rhs = lax.optimization_barrier((value, rhs))
    _, r1, r2, r2_own = steps
    inverse = None
    if eliminating:
        r2, own, got = lax.optimization_barrier((r2, own, got))
        r2, state = in_between(r2, [scaled], (0, 40))
    r3 = cross(add_last(own, got, r1, r2), 2)
    if eliminating:
        r3, (inverse,) = in_between(r3, state, (40, 128))
    return sum_rows([own, got, r1, r2_own, r3], inverse)


def gather_rows(dev, own):
    p = [own] + [None] * 7
    for a, step in ((0, 2), (0, 1), (0, 0), (1, 1), (1, 0), (2, 0), (3, 0)):
        at = a | (4 >> step)
        p[at] = cross(p[a], step)

    def body(dev, *refs):
        for at in range(CHIPS):
            to = piece_at(NEAR_LINKS, core_of(dev), near_of(dev), at)
            refs[-1][to] = refs[at][0]

    pieces = ((CHIPS, PIECE, K), F32)
    return kernel_call(body, [pieces], [dev], [], p)[0].reshape(HALF, K)


def shards(pair_coeffs, pair_gaps, trial_vectors):
    dev = lax.axis_index(("z", "xl", "c") + AUX).astype(jnp.int32)[None]
    gaps = pair_gaps.reshape(CHIPS, PAIRS_J)
    dev, gaps, trial_vectors = lax.optimization_barrier((dev, gaps, trial_vectors))
    bhi, blo, parts = first_projection(pair_coeffs, trial_vectors)
    for step in range(2):
        scaled = to_each(sum_aux(dev, to_each(parts, AUX), gaps), AUX)
        mine = gather_rows(dev, reduce_rows(dev, bhi, blo, scaled, step == 1))
        theirs = exchange(mine, "c", 1)
        so_far = project_half(dev, bhi, blo, mine, None)
        parts, *rest = project_half(dev, bhi, blo, theirs, so_far, step == 1)
    total, gram = add_over_cores(dev, reduce_aux(dev, parts, *rest, gaps))
    state = [gram]
    for axis, cut in (("z", (0, 40)), ("y", (40, 84)), (("xl", "xh"), None)):
        got = []
        for mask in (1, 2, 3):
            got.append(exchange(total, axis, mask))
        if cut:
            got, state = in_between(got, state, cut)
            total = (total + got[0]) + (got[1] + got[2])
    vectors_out, inverse = finish(dev, mine, theirs, state, 84)
    rayleigh = rayleigh_matrix(inverse, [total, *got])
    return vectors_out, rayleigh


def solution(mesh):
    cube = Mesh(mesh.devices.reshape(4, 2, 2, 2, 4), ("z", "xl", "c", "xh", "y"))

    return jax.shard_map(
        shards,
        mesh=cube,
        in_specs=(P(AUX, ("z", "xl", "c")), P(("z", "xl", "c")), P(AUX, None)),
        out_specs=(P(AUX, None), P()),
        check_vma=False,
    )
```

```python
import itertools

import jax
import jax.numpy as jnp
from jax import lax
from jax.experimental import pallas as pl
from jax.experimental.pallas import tpu as pltpu
from jax.sharding import Mesh, PartitionSpec as P


F32 = jnp.float32
BF16 = jnp.bfloat16
HIGHEST = lax.Precision.HIGHEST

NAUX_L = 4500
PAIRS_L = 1024
K = 128
CHUNK = 768
CHUNKS = 6
ROWS = CHUNK * CHUNKS
HALF = ROWS // 2
TAIL = NAUX_L - CHUNK * (CHUNKS - 1)
CHIPS = 8
PIECE = HALF // CHIPS
PAIRS_J = PAIRS_L // CHIPS
GRAM_J = K // CHIPS


def split(x):
    hi = x.astype(BF16)
    return hi, (x - hi.astype(F32)).astype(BF16)


def dot(a, b, ca, cb, precision=None):
    return lax.dot_general(
        a, b, (((ca,), (cb,)), ((), ())), precision=precision, preferred_element_type=F32
    )


VMEM_SPEC = pl.BlockSpec(memory_space=pltpu.VMEM)


def cost(us):
    return pl.CostEstimate(flops=int(us * 1.5e8), bytes_accessed=0, transcendentals=0)


def core_of(dev):
    return (dev[0] >> 3) & 1


def near_of(dev):
    return ((dev[0] >> 4) & 1) * 4 + (dev[0] >> 5)


def aux_of(dev):
    return dev[0] & 7


def kernel_call(body, outs, smem, hbm, vmem, scratch=(), limit=12 << 20, us=0.3):
    return pl.pallas_call(
        body,
        out_shape=[pltpu.VMEM(s, d) for s, d in outs],
        in_specs=[pl.BlockSpec(memory_space=pltpu.SMEM)] * len(smem)
        + [pl.BlockSpec(memory_space=pl.ANY)] * len(hbm)
        + [VMEM_SPEC] * len(vmem),
        out_specs=[VMEM_SPEC] * len(outs),
        scratch_shapes=list(scratch),
        compiler_params=pltpu.CompilerParams(vmem_limit_bytes=limit),
        cost_estimate=cost(us),
    )(*smem, *hbm, *[pltpu.with_memory_space_constraint(v, pltpu.VMEM) for v in vmem])


MASK = {("z", 1): 1, ("z", 3): 3, ("xl", 1): 4, ("y", 1): 1, ("y", 3): 3, ("xh", 1): 4}
NEAR_LINKS = ((("z", 1), ("z", 3), ("xl", 1)), (("xl", 1), ("z", 1), ("z", 3)))
AUX_LINKS = ((("y", 1), ("y", 3), ("xh", 1)), (("y", 3), ("y", 1), ("xh", 1)))


def piece_at(links, core, me, p):
    masks = [0, 0]
    for c in range(2):
        for t in range(3):
            if (p >> (2 - t)) & 1:
                masks[c] ^= MASK[links[c][t]]
    return me ^ jnp.where(core == 0, masks[0], masks[1])


def transposed_halves(v):
    hi, lo = split(v.T)
    return jnp.concatenate([hi, lo], axis=0)


def fold(x):
    return x[0:K, :] + x[K : 2 * K, :]


def first_projection(coeffs, vectors):
    def body(b_hbm, v_hbm, bhi, blo, out, bbuf, vbuf, btail, vtail, sems):
        def copies(i):
            last = i == CHUNKS - 1
            rows = pl.ds(i * CHUNK, TAIL if last else CHUNK)
            return (
                pltpu.make_async_copy(b_hbm.at[rows], btail if last else bbuf.at[i], sems.at[0, i]),
                pltpu.make_async_copy(v_hbm.at[rows], vtail if last else vbuf.at[i], sems.at[1, i]),
            )

        for i in range(CHUNKS):
            for c in copies(i):
                c.start()

        def chunk(slot, row0):
            vt = transposed_halves(vbuf[slot])
            for n in range(4):
                hi, lo = split(bbuf[slot, :, 256 * n : 256 * n + 256])
                bhi[n, pl.ds(row0, CHUNK), :] = hi
                blo[n, pl.ds(row0, CHUNK), :] = lo
                part = fold(dot(vt, hi, 1, 0)) + dot(vt[0:K], lo, 1, 0)
                for t in range(2):
                    out[2 * n + t] += part[:, 128 * t : 128 * t + 128]

        out[...] = jnp.zeros(out.shape, F32)

        def middle(i, carry):
            rows = pl.ds(pl.multiple_of(i * CHUNK, CHUNK), CHUNK)
            pltpu.make_async_copy(b_hbm.at[rows], bbuf.at[i], sems.at[0, i]).wait()
            pltpu.make_async_copy(v_hbm.at[rows], vbuf.at[i], sems.at[1, i]).wait()
            chunk(i, pl.multiple_of(i * CHUNK, CHUNK))
            return carry

        lax.fori_loop(0, CHUNKS - 1, middle, 0)
        for c in copies(CHUNKS - 1):
            c.wait()
        whole = TAIL // 8 * 8
        bbuf[0, whole:, :] = jnp.zeros((CHUNK - whole, PAIRS_L), F32)
        vbuf[0, whole:, :] = jnp.zeros((CHUNK - whole, K), F32)
        bbuf[0, 0:TAIL, :] = btail[...]
        vbuf[0, 0:TAIL, :] = vtail[...]
        chunk(0, CHUNK * (CHUNKS - 1))

    halves = ((4, ROWS, 256), BF16)
    coeffs = pltpu.with_memory_space_constraint(coeffs, pltpu.HBM)
    vectors = pltpu.with_memory_space_constraint(vectors, pltpu.HBM)
    return kernel_call(
        body,
        [halves, halves, ((CHIPS, K, PAIRS_J), F32)],
        [],
        [coeffs, vectors],
        [],
        scratch=[
            pltpu.VMEM((CHUNKS - 1, CHUNK, PAIRS_L), F32),
            pltpu.VMEM((CHUNKS - 1, CHUNK, K), F32),
            pltpu.VMEM((TAIL, PAIRS_L), F32),
            pltpu.VMEM((TAIL, K), F32),
            pltpu.SemaphoreType.DMA((2, CHUNKS)),
        ],
        limit=26 << 20,
        us=8.0,
    )


def project_half(dev, bhi, blo, v, so_far, by_position=False):
    def body(dev, bhi, blo, v, *rest):
        if so_far is None:
            acc, gacc = rest
            half = core_of(dev)
        else:
            acc0, gacc0, *outs, acc, gacc = rest
            half = 1 - core_of(dev)
        for i in range(3):
            row0 = pl.multiple_of(half * HALF + i * CHUNK, CHUNK)
            vt = transposed_halves(v[CHUNK * i : CHUNK * (i + 1), :])
            for n in range(4):
                part = fold(dot(vt, bhi[n, pl.ds(row0, CHUNK), :], 1, 0))
                part = part + dot(vt[0:K], blo[n, pl.ds(row0, CHUNK), :], 1, 0)
                for t in range(2):
                    value = part[:, 128 * t : 128 * t + 128]
                    j = 2 * n + t
                    if i > 0:
                        value = acc[j] + value
                    if so_far is not None and i == 2:
                        value = acc0[j] + value
                    acc[j] = value
            g = dot(vt, vt, 1, 1)
            gacc[...] = g if i == 0 else gacc[...] + g
        if so_far is not None:
            g = gacc[...] + gacc0[...]
            gram = (g[0:K, 0:K] + g[K:, K:]) + (g[0:K, K:] + g[K:, 0:K])
            if by_position:
                for out, places in zip(outs, ((6, 7), (4, 5), (0, 1, 2, 3))):
                    for t, p in enumerate(places):
                        out[t] = acc[piece_at(AUX_LINKS, core_of(dev), aux_of(dev), p)]
                outs[0][2] = gram
                outs[2][4] = gram
            else:
                for j in range(CHIPS):
                    outs[0][j, 0:K, :] = acc[j]
                    outs[0][j, K:, :] = gram[GRAM_J * j : GRAM_J * (j + 1), :]

    acc = ((CHIPS, K, PAIRS_J), F32)
    gacc = ((2 * K, 2 * K), F32)
    if so_far is None:
        return kernel_call(body, [acc, gacc], [dev], [], [bhi, blo, v], us=3.0)
    return kernel_call(
        body,
        [((n, K, K), F32) for n in (3, 2, 5)]
        if by_position
        else [((CHIPS, K + GRAM_J, PAIRS_J), F32)],
        [dev],
        [],
        [bhi, blo, v, *so_far],
        scratch=[pltpu.VMEM(*acc), pltpu.VMEM(*gacc)],
        us=3.0,
    )


def weights_of(dev, gaps):
    gap = gaps[pl.ds(aux_of(dev), 1), :]
    return 4.0 * gap / (gap * gap + 1.0)


def sum_aux(dev, parts, gaps):
    def body(dev, p, gaps, out):
        s = ((p[0] + p[1]) + (p[2] + p[3])) + ((p[4] + p[5]) + (p[6] + p[7]))
        piece = s[0:K] * weights_of(dev, gaps)
        for j in range(CHIPS):
            out[j, 0:K, :] = piece
            if p.shape[1] > K:
                out[j, K:, :] = s[K:]

    return kernel_call(body, [(parts.shape, F32)], [dev], [], [parts, gaps])[0]


def reduce_aux(dev, early, late, keep, gaps):
    def second_step(k, ra, first, other):
        first[0] = k[3] + ra[1]
        first[1] = k[4] + ra[2]
        other[0] = k[2] + ra[0]

    def last_step(k, ra, rb, r2, out):
        out[0] = (k[1] + rb[1]) + r2[0]
        out[1] = (k[4] + ra[2]) + r2[1]

    def finish_sum(dev, k, ra, rb, r2, r2_own, r3, gaps, out):
        own = ((k[0] + rb[0]) + r2_own[0]) + r3[0]
        out[0] = dot(own * weights_of(dev, gaps), own, 1, 1, HIGHEST)
        out[1] = ((k[4] + ra[2]) + r2[1]) + r3[1]

    def pieces(n):
        return [((n, K, K), F32)]

    ra = cross(early, 0, AUX_LINKS)
    rb = cross(late, 0, AUX_LINKS)
    first, other = kernel_call(second_step, pieces(2) + pieces(1), [], [], [keep, ra])
    r2 = cross(first, 1, AUX_LINKS)
    r2_own = cross(other, 1, AUX_LINKS)
    (send,) = kernel_call(last_step, pieces(2), [], [], [keep, ra, rb, r2])
    r3 = cross(send, 2, AUX_LINKS)
    ins = [keep, ra, rb, r2, r2_own, r3, gaps]
    return kernel_call(finish_sum, pieces(2), [dev], [], ins)[0]


def add_over_cores(dev, both):
    def body(dev, own, got, total, gram):
        total[...] = own[0] + got[0]
        gram[...] = jnp.where(core_of(dev) == 1, own[1], got[1])

    got = exchange(both, "c", 1)
    return kernel_call(body, [((K, K), F32)] * 2, [dev], [], [both, got])


def apply_pieces(dev, bhi, blo, scaled, other, make_rhs, first):
    def body(dev, bhi, blo, s, out, *rest):
        if make_rhs:
            st = rest[0]
            for j in range(CHIPS):
                hi, lo = split(s[j, 0:K, :])
                lanes = slice(128 * (j % 2), 128 * (j % 2) + 128)
                st[j // 2, 0:K, lanes] = hi
                st[j // 2, K : 2 * K, lanes] = lo
        else:
            st = s
        core = core_of(dev)
        if other:
            core = 1 - core

        for i in range(2):
            start = core * HALF + piece_at(NEAR_LINKS, core, near_of(dev), first + i) * PIECE
            start = pl.multiple_of(start, PIECE)
            res = None
            for ref in (bhi, blo):
                for n in range(4):
                    d = dot(ref[n, pl.ds(start, PIECE), :], st[n], 1, 1)
                    res = d if res is None else res + d
            out[i] = res[:, 0:K] + res[:, K : 2 * K]

    outs = [((2, PIECE, K), F32)]
    if make_rhs:
        outs.append(((4, 2 * K, 256), BF16))
    return kernel_call(body, outs, [dev], [], [bhi, blo, scaled], us=0.75)


def add_slots(first, count, *parts):
    def body(*refs):
        total = refs[0][first : first + count]
        for r in refs[1:-1]:
            total = total + r[first : first + count]
        refs[-1][...] = total

    shape = (count, *parts[0].shape[1:])
    return kernel_call(body, [(shape, F32)], [], [], list(parts))[0]


def add_last(own, got, r1, r2):
    def body(own, got, r1, r2, out):
        out[0] = ((own[1] + got[1]) + r1[1]) + r2[0]

    return kernel_call(body, [((1, PIECE, K), F32)], [], [], [own, got, r1, r2])[0]


def sum_rows(parts, inverse):
    def body(*refs):
        out = refs[-1]
        own, got, r1, r2, r3 = refs[:5]
        s = ((own[0] + got[0]) + r1[0]) + (r2[0] + r3[0])
        if inverse is not None:
            s = dot(s, refs[len(parts)][...], 1, 1, HIGHEST)
        out[0] = s

    extra = [] if inverse is None else [inverse]
    return kernel_call(body, [((1, PIECE, K), F32)], [], [], [*parts, *extra])[0]


def pivots(gs, ws, begin, end):
    lane = lax.broadcasted_iota(jnp.int32, (K, K), 1)
    sub = lax.broadcasted_iota(jnp.int32, (K, K), 0)

    def step(h, low):
        k = 4 * h
        lanes, rows = lane[low:], sub[low:, 0:1]
        g, w_all = gs[low:, :], ws[low:, :]

        def pick(x, at):
            return jnp.sum(jnp.where(lanes[0 : x.shape[0]] == at, x, 0.0), axis=1, keepdims=True)

        r = [gs[pl.ds(k + i, 1), :] for i in range(4)]
        w = [ws[pl.ds(k + i, 1), :] for i in range(4)]
        c = [pick(g, k + i) for i in range(4)]
        d = [[pick(r[i], k + t) for t in range(4)] for i in range(4)]
        for i in range(4):
            inv = 1.0 / d[i][i]
            f = jnp.where(rows > k + i, c[i] * inv, 0.0)
            for t in range(i + 1, 4):
                c[t] = c[t] - f * d[i][t]
                m = d[t][i] * inv
                r[t] = r[t] - m * r[i]
                w[t] = w[t] - m * w[i]
                for u in range(i + 1, 4):
                    d[t][u] = d[t][u] - m * d[i][u]
            g = g - f * r[i]
            w_all = w_all - f * w[i]
        gs[low:, :] = g
        ws[low:, :] = w_all

    for low, top in ((0, 64), (64, K)):
        one, last = max(begin, low), min(end, top)
        if one < last:
            lax.fori_loop(one // 4, last // 4, lambda h, c, low=low: (step(h, low), c)[1], 0)


def scaled_rows(gs, ws):
    lane = lax.broadcasted_iota(jnp.int32, (K, K), 1)
    sub = lax.broadcasted_iota(jnp.int32, (K, K), 0)
    d = jnp.sum(jnp.where(lane == sub, gs[...], 0.0), axis=1, keepdims=True)
    return ws[...] / jnp.sqrt(d)


def eliminate(state, begin, end):
    start, stop = begin == 0, end == K

    def body(*refs):
        gs, ws = refs[-2:]
        if start:
            g_ref = refs[0]
            if len(g_ref.shape) == 2:
                gs[...] = g_ref[...]
            else:
                row0 = g_ref.shape[1] - GRAM_J
                for j in range(CHIPS):
                    gs[GRAM_J * j : GRAM_J * (j + 1), :] = g_ref[j, row0:, :]
            lane = lax.broadcasted_iota(jnp.int32, (K, K), 1)
            sub = lax.broadcasted_iota(jnp.int32, (K, K), 0)
            ws[...] = jnp.where(lane == sub, 1.0, 0.0).astype(F32)
        else:
            gs[...] = refs[0][...]
            ws[...] = refs[1][...]
        pivots(gs, ws, begin, end)
        if stop:
            refs[-3][...] = scaled_rows(gs, ws)

    square = ((K, K), F32)
    if stop:
        outs, scratch = [square], [pltpu.VMEM(*square), pltpu.VMEM(*square)]
    else:
        outs, scratch = [square, square], []
    return kernel_call(body, outs, [], [], list(state), scratch=scratch, us=(end - begin) / 20)


def in_between(value, state, cuts):
    state = eliminate(state, cuts[0], cuts[1])
    value, *state = lax.optimization_barrier((value, *state))
    return value, state


def finish(dev, mine, theirs, state, begin):
    def body(dev, mine, theirs, g, w, out, inv, gs, ws, both, buf, tail, sem):
        gs[...] = g[...]
        ws[...] = w[...]
        pivots(gs, ws, begin, K)
        inv[...] = scaled_rows(gs, ws)
        both[core_of(dev)] = mine[...]
        both[1 - core_of(dev)] = theirs[...]
        ihi, ilo = split(inv[...])
        rhs = jnp.concatenate([ihi, ilo], axis=0)

        def copy(i):
            last = i == CHUNKS - 1
            rows = pl.ds(i * CHUNK, TAIL if last else CHUNK)
            return pltpu.make_async_copy(tail if last else buf.at[i], out.at[rows], sem.at[i])

        for i in range(CHUNKS):
            start = CHUNK * (i % 3)
            vhi, vlo = split(both[i // 3, start : start + CHUNK, :])
            r = dot(vhi, rhs, 1, 1) + dot(vlo, rhs, 1, 1)
            r = r[:, 0:K] + r[:, K : 2 * K]
            if i == CHUNKS - 1:
                tail[...] = r[0:TAIL]
            else:
                buf[i] = r
            copy(i).start()
        for i in range(CHUNKS):
            copy(i).wait()

    square = pltpu.VMEM((K, K), F32)
    return pl.pallas_call(
        body,
        out_shape=[jax.ShapeDtypeStruct((NAUX_L, K), F32), square],
        in_specs=[pl.BlockSpec(memory_space=pltpu.SMEM)] + [VMEM_SPEC] * 4,
        out_specs=[pl.BlockSpec(memory_space=pl.ANY), VMEM_SPEC],
        scratch_shapes=[
            square,
            square,
            pltpu.VMEM((2, HALF, K), F32),
            pltpu.VMEM((CHUNKS - 1, CHUNK, K), F32),
            pltpu.VMEM((TAIL, K), F32),
            pltpu.SemaphoreType.DMA((CHUNKS,)),
        ],
        compiler_params=pltpu.CompilerParams(vmem_limit_bytes=16 << 20),
        cost_estimate=cost(4.2),
        name="finish",
    )(dev, *[pltpu.with_memory_space_constraint(v, pltpu.VMEM) for v in (mine, theirs, *state)])


def rayleigh_matrix(inverse, parts):
    def body(inv, a, b, c, d, out):
        total = (a[...] + b[...]) + (c[...] + d[...])
        out[...] = dot(dot(inv[...], total, 1, 0, HIGHEST), inv[...], 1, 1, HIGHEST)

    return kernel_call(body, [((K, K), F32)], [], [], [inverse, *parts])[0]


def exchange(value, axis, mask):
    n = lax.axis_size(axis)
    return lax.ppermute(value, axis, [(i, i ^ mask) for i in range(n)])


def to_each(value, axes):
    return lax.all_to_all(value, axes, split_axis=0, concat_axis=0, tiled=True)


AUX = ("xh", "y")


def cross(value, step, links=NEAR_LINKS):
    axes = ("z", "xl", "c") if links is NEAR_LINKS else ("c", "xh", "y")
    sizes = [lax.axis_size(a) for a in axes]
    pairs = []
    for at in itertools.product(*map(range, sizes)):
        to = dict(zip(axes, at))
        axis, mask = links[to["c"]][step]
        to[axis] ^= mask
        ids = [(a * sizes[1] + b) * sizes[2] + c for a, b, c in (at, tuple(to.values()))]
        pairs.append(tuple(ids))
    return lax.ppermute(value, axes, pairs)


def reduce_rows(dev, bhi, blo, scaled, eliminating):
    rhs = None

    def apply_pair(first):
        nonlocal rhs
        send, *made = apply_pieces(
            dev, bhi, blo, scaled if rhs is None else rhs, True, rhs is None, first
        )
        rhs = made[0] if made else rhs
        got = exchange(send, "c", 1)
        (own,) = apply_pieces(dev, bhi, blo, rhs, False, False, first)
        return own, got

    steps = []
    for first in (6, 4, 2, 0):
        own, got = apply_pair(first)
        if first == 0:
            break
        if first > 2:
            value = add_slots(0, 2, own, got)
            steps.append(cross(value, 0))
        else:
            for slot in (1, 0):
                value = add_slots(slot, 1, own, got, steps[0])
                steps.append(cross(value, 1))
        value, rhs = lax.optimization_barrier((value, rhs))
    _, r1, r2, r2_own = steps
    inverse = None
    if eliminating:
        r2, own, got = lax.optimization_barrier((r2, own, got))
        r2, state = in_between(r2, [scaled], (0, 40))
    r3 = cross(add_last(own, got, r1, r2), 2)
    if eliminating:
        r3, (inverse,) = in_between(r3, state, (40, 128))
    return sum_rows([own, got, r1, r2_own, r3], inverse)


def gather_rows(dev, own):
    p = [own] + [None] * 7
    for a, step in ((0, 2), (0, 1), (0, 0), (1, 1), (1, 0), (2, 0), (3, 0)):
        at = a | (4 >> step)
        p[at] = cross(p[a], step)

    def body(dev, *refs):
        for at in range(CHIPS):
            to = piece_at(NEAR_LINKS, core_of(dev), near_of(dev), at)
            refs[-1][to] = refs[at][0]

    pieces = ((CHIPS, PIECE, K), F32)
    return kernel_call(body, [pieces], [dev], [], p)[0].reshape(HALF, K)


def shards(pair_coeffs, pair_gaps, trial_vectors):
    dev = lax.axis_index(("z", "xl", "c") + AUX).astype(jnp.int32)[None]
    gaps = pair_gaps.reshape(CHIPS, PAIRS_J)
    dev, gaps, trial_vectors = lax.optimization_barrier((dev, gaps, trial_vectors))
    bhi, blo, parts = first_projection(pair_coeffs, trial_vectors)
    for step in range(2):
        scaled = to_each(sum_aux(dev, to_each(parts, AUX), gaps), AUX)
        mine = gather_rows(dev, reduce_rows(dev, bhi, blo, scaled, step == 1))
        theirs = exchange(mine, "c", 1)
        so_far = project_half(dev, bhi, blo, mine, None)
        parts, *rest = project_half(dev, bhi, blo, theirs, so_far, step == 1)
    total, gram = add_over_cores(dev, reduce_aux(dev, parts, *rest, gaps))
    state = [gram]
    for axis, cut in (("z", (0, 40)), ("y", (40, 84)), (("xl", "xh"), None)):
        got = []
        for mask in (1, 2, 3):
            got.append(exchange(total, axis, mask))
        if cut:
            got, state = in_between(got, state, cut)
            total = (total + got[0]) + (got[1] + got[2])
    vectors_out, inverse = finish(dev, mine, theirs, state, 84)
    rayleigh = rayleigh_matrix(inverse, [total, *got])
    return vectors_out, rayleigh


def solution(mesh):
    cube = Mesh(mesh.devices.reshape(4, 2, 2, 2, 4), ("z", "xl", "c", "xh", "y"))

    return jax.shard_map(
        shards,
        mesh=cube,
        in_specs=(P(AUX, ("z", "xl", "c")), P(("z", "xl", "c")), P(AUX, None)),
        out_specs=(P(AUX, None), P()),
        check_vma=False,
    )
```
